8 devices in a mesh: fsdp: 2 (over z, y), ep: 4 (over x, core).
Axes of the slice: x: 2, y: 2, z: 1, core: 2. Of those that a mesh axis runs over, the one named last changes fastest.
Arguments:
- x_tok: bfloat16 [16384, 512], P(('fsdp', 'ep'))
- dy_tok: bfloat16 [16384, 512], P(('fsdp', 'ep'))
- expert_ids: int32 [16384, 6], P(('fsdp', 'ep'))
- route_w: float32 [16384, 6], P(('fsdp', 'ep'))
- w_gate: bfloat16 [64, 512, 1408], P('ep', 'fsdp')
- w_up: bfloat16 [64, 512, 1408], P('ep', 'fsdp')
- w_down: bfloat16 [64, 1408, 512], P('ep', None, 'fsdp')
Outputs:
- output 1: bfloat16 [16384, 512], P(('fsdp', 'ep'))
- output 2: float32 [16384, 6], P(('fsdp', 'ep'))
- output 3: float32 [64, 512, 1408], P('ep', 'fsdp')
- output 4: float32 [64, 512, 1408], P('ep', 'fsdp')
- output 5: float32 [64, 1408, 512], P('ep', None, 'fsdp')
All inputs are finite; a program needn't handle non-finite values.
Results may differ from the reference program's by a relative error of at most 0.00900672.
Values are sent between devices in bfloat16 or wider.
A program may use at most 1 GiB of HBM per device.

```python
import jax
import jax.numpy as jnp
from jax import lax

D_MODEL = 512
D_FF = 1408
EXPERTS = 64
TOP_K = 6
TOK_DEV = 2048
DEVICES = 8
CAPACITY = 576

TOKENS = DEVICES * TOK_DEV
SLOTS = EXPERTS * CAPACITY
HOT_COUNT = max(1, TOP_K // 2)


def draw_routing(root_key):
    key_hot, key_score = jax.random.split(root_key)
    hot_rank = jax.random.permutation(key_hot, EXPERTS)
    bias = jnp.where(hot_rank < HOT_COUNT, 768, 0).astype(jnp.int32)
    expert_col = jnp.arange(EXPERTS, dtype=jnp.int32)

    def one_device(dev_key):
        noise = jax.random.randint(dev_key, (TOK_DEV, EXPERTS), 0, 1024, dtype=jnp.int32)
        score = (noise + bias[None, :]) * EXPERTS + expert_col[None, :]
        return lax.top_k(score, TOP_K)[1]

    chosen = lax.map(one_device, jax.random.split(key_score, DEVICES))
    return chosen.reshape(TOKENS, TOP_K).astype(jnp.int32)


def setup_inputs(seed: int = 0) -> dict:
    key_list = jax.random.split(jax.random.key(seed), 7)
    x_tok = jax.random.normal(key_list[0], (TOKENS, D_MODEL), jnp.float32)
    dy_tok = jax.random.normal(key_list[1], (TOKENS, D_MODEL), jnp.float32)
    expert_ids = draw_routing(key_list[2])
    route_w = jax.random.uniform(key_list[3], (TOKENS, TOP_K), jnp.float32, 0.1, 1.0)
    w_gate = jax.random.normal(key_list[4], (EXPERTS, D_MODEL, D_FF), jnp.float32) * D_MODEL ** -0.5
    w_up = jax.random.normal(key_list[5], (EXPERTS, D_MODEL, D_FF), jnp.float32) * D_MODEL ** -0.5
    w_down = jax.random.normal(key_list[6], (EXPERTS, D_FF, D_MODEL), jnp.float32) * D_FF ** -0.5
    return {
        "x_tok": x_tok.astype(jnp.bfloat16),
        "dy_tok": dy_tok.astype(jnp.bfloat16),
        "expert_ids": expert_ids,
        "route_w": route_w,
        "w_gate": w_gate.astype(jnp.bfloat16),
        "w_up": w_up.astype(jnp.bfloat16),
        "w_down": w_down.astype(jnp.bfloat16),
    }


def slot_positions(ids_dev):
    onehot = (ids_dev[:, None] == jnp.arange(EXPERTS, dtype=jnp.int32)[None, :]).astype(jnp.int32)
    before = jnp.cumsum(onehot, axis=0) - onehot
    position = jnp.sum(before * onehot, axis=1)
    return jnp.where(position < CAPACITY, ids_dev * CAPACITY + position, SLOTS)


def swiglu_grads(pre_gate, pre_up, grad_hidden):
    sigma = jax.nn.sigmoid(pre_gate)
    grad_gate = grad_hidden * pre_up * sigma * (1.0 + pre_gate * (1.0 - sigma))
    grad_up = grad_hidden * pre_gate * sigma
    return grad_gate.astype(jnp.bfloat16), grad_up.astype(jnp.bfloat16)


def reference(x_tok, dy_tok, expert_ids, route_w, w_gate, w_up, w_down):
    dest_slot = lax.map(slot_positions, expert_ids.reshape(DEVICES, TOK_DEV * TOP_K))
    pair_ids = jnp.arange(TOKENS * TOP_K, dtype=jnp.int32).reshape(DEVICES, TOK_DEV * TOP_K)
    dev_rows = jnp.broadcast_to(jnp.arange(DEVICES, dtype=jnp.int32)[:, None], dest_slot.shape)
    slot_src = jnp.full((DEVICES, SLOTS + 1), TOKENS * TOP_K, jnp.int32)
    slot_src = slot_src.at[dev_rows, dest_slot].set(pair_ids)[:, :SLOTS]
    per_expert = slot_src.reshape(DEVICES, EXPERTS, CAPACITY).transpose(1, 0, 2).reshape(EXPERTS, DEVICES * CAPACITY)
    route_flat = route_w.reshape(-1)

    def expert_step(carry, step_in):
        dx_acc, dr_acc = carry
        pair_src, w_gate_e, w_up_e, w_down_e = step_in
        tok_rows = pair_src // TOP_K
        x_rows = jnp.take(x_tok, tok_rows, axis=0, mode="fill", fill_value=0)
        dy_rows = jnp.take(dy_tok, tok_rows, axis=0, mode="fill", fill_value=0)
        gate_rows = jnp.take(route_flat, pair_src, axis=0, mode="fill", fill_value=0)
        pre_gate = jnp.dot(x_rows, w_gate_e, preferred_element_type=jnp.float32)
        pre_up = jnp.dot(x_rows, w_up_e, preferred_element_type=jnp.float32)
        hidden = (jax.nn.silu(pre_gate) * pre_up).astype(jnp.bfloat16)
        y_rows = jnp.dot(hidden, w_down_e, preferred_element_type=jnp.float32)
        dy_wide = dy_rows.astype(jnp.float32)
        scaled_dy = (gate_rows[:, None] * dy_wide).astype(jnp.bfloat16)
        dr_rows = jnp.sum(dy_wide * y_rows, axis=1)
        grad_hidden = jnp.dot(scaled_dy, w_down_e.T, preferred_element_type=jnp.float32)
        grad_gate, grad_up = swiglu_grads(pre_gate, pre_up, grad_hidden)
        dx_rows = (jnp.dot(grad_gate, w_gate_e.T, preferred_element_type=jnp.float32)
                   + jnp.dot(grad_up, w_up_e.T, preferred_element_type=jnp.float32)).astype(jnp.bfloat16)
        dw_gate = jnp.dot(x_rows.T, grad_gate, preferred_element_type=jnp.float32)
        dw_up = jnp.dot(x_rows.T, grad_up, preferred_element_type=jnp.float32)
        dw_down = jnp.dot(hidden.T, scaled_dy, preferred_element_type=jnp.float32)
        dx_acc = dx_acc.at[tok_rows].add(dx_rows.astype(jnp.float32), mode="drop")
        dr_acc = dr_acc.at[pair_src].set(dr_rows, mode="drop")
        return (dx_acc, dr_acc), (dw_gate, dw_up, dw_down)

    init = (jnp.zeros((TOKENS, D_MODEL), jnp.float32), jnp.zeros((TOKENS * TOP_K,), jnp.float32))
    (dx_acc, dr_acc), (grad_w_gate, grad_w_up, grad_w_down) = lax.scan(
        expert_step, init, (per_expert, w_gate, w_up, w_down))
    grad_x = dx_acc.astype(jnp.bfloat16)
    route_w_grad = dr_acc.reshape(TOKENS, TOP_K)
    return (grad_x, route_w_grad, grad_w_gate, grad_w_up, grad_w_down)
```

```python
import functools

import jax
import jax.numpy as jnp
from jax import lax
from jax.experimental import pallas as pl
from jax.experimental.pallas import tpu as pltpu
from jax.sharding import PartitionSpec as P

CAP_FACTOR = 3
CHUNKS = 4
GROUPS = (5, 5, 4, 2)
LANES = 128
SUB = 8
INTERPRET = False


def capacity_of(tok_dev, top_k, experts):
    return max(8, ((CAP_FACTOR * tok_dev * top_k // experts + 7) // 8) * 8)


def route_kernel(n_pairs, top_k, experts, capacity, ids_ref, gate_ref, tok_ref, slot_gate_ref, cnt_ref):
    for e in range(experts):
        cnt_ref[e] = 0

    def step(t, carry):
        for j in range(top_k):
            e = ids_ref[t * top_k + j]
            n = cnt_ref[e]

            @pl.when(n < capacity)
            def _():
                slot = e * capacity + n
                tok_ref[slot] = t
                slot_gate_ref[slot] = gate_ref[t * top_k + j]
                cnt_ref[e] = n + 1
        return carry

    lax.fori_loop(0, n_pairs // top_k, step, 0)


def route_slots(ids_flat, gates_flat, top_k, experts, capacity):
    n_pairs = ids_flat.shape[0]
    smem = pl.BlockSpec(memory_space=pltpu.SMEM)
    return pl.pallas_call(
        functools.partial(route_kernel, n_pairs, top_k, experts, capacity),
        in_specs=[smem, smem],
        out_specs=[smem, smem, smem],
        out_shape=[
            jax.ShapeDtypeStruct((experts * capacity,), jnp.int32),
            jax.ShapeDtypeStruct((experts * capacity,), jnp.float32),
            jax.ShapeDtypeStruct((experts,), jnp.int32),
        ],
        name="route",
        interpret=INTERPRET,
    )(ids_flat, gates_flat)


def gather_kernel(n_src, exp_local, capacity, chunk, cnt_ref, nt_ref, tok_ref, gate_ref, *refs):
    token_refs = refs[:n_src]
    xg_hbm, dy_hbm, rows_v, buf_x, buf_g, xg_v, dy_v, xg_sem, dy_sem, tok_sem = refs[n_src:]
    src = pl.program_id(0)
    half = n_src // 2
    for k in range(n_src):
        @pl.when(src == k)
        def _(k=k):
            copy = pltpu.make_async_copy(token_refs[k], rows_v, tok_sem)
            copy.start()
            copy.wait()
    region = src // half
    lane_src = src % half

    def xg_copy(e, j, slot):
        return pltpu.make_async_copy(
            xg_v.at[slot], xg_hbm.at[e, region, j, pl.ds(lane_src * chunk, chunk)], xg_sem.at[slot])

    def dy_copy(e, j, slot):
        return pltpu.make_async_copy(
            dy_v.at[slot], dy_hbm.at[e, j, pl.ds(lane_src * chunk, chunk)], dy_sem.at[slot])

    def one_expert(e, done):
        n = cnt_ref[src * exp_local + e]

        def one_chunk(j, done):
            slot = lax.rem(done, 2)

            @pl.when(done >= 2)
            def _():
                xg_copy(e, j, slot).wait()

                @pl.when(region == 0)
                def _():
                    dy_copy(e, j, slot).wait()

            def rows(r8, carry):
                for u in range(8):
                    r = r8 * 8 + u
                    pos = j * chunk + r
                    ok = pos < n
                    t = jnp.where(ok, tok_ref[0, 0, e * capacity + pos], 0)
                    w = jnp.where(ok, gate_ref[0, 0, e * capacity + pos], 0.0)
                    row = rows_v[t].astype(jnp.float32)
                    at = pl.ds(pl.multiple_of(r * SUB, SUB), SUB)
                    buf_x[at, :] = row
                    buf_g[at, :] = row * w
                return carry

            lax.fori_loop(0, chunk // 8, rows, 0)
            for c in range(SUB // 2):
                xg_v[slot, :, c * LANES:(c + 1) * LANES] = buf_x[pl.ds(c, chunk, stride=SUB), :].astype(jnp.bfloat16)
                g_c = buf_g[pl.ds(SUB // 2 + c, chunk, stride=SUB), :]
                xg_v[slot, :, (SUB // 2 + c) * LANES:(SUB // 2 + c + 1) * LANES] = g_c.astype(jnp.bfloat16)
            xg_copy(e, j, slot).start()

            @pl.when(region == 0)
            def _():
                for c in range(SUB // 2):
                    d_c = buf_x[pl.ds(SUB // 2 + c, chunk, stride=SUB), :]
                    dy_v[slot, :, c * LANES:(c + 1) * LANES] = d_c.astype(jnp.bfloat16)
                dy_copy(e, j, slot).start()
            return done + 1

        return lax.fori_loop(0, nt_ref[e * 2 + region], one_chunk, done)

    lax.fori_loop(0, exp_local, one_expert, 0)
    for slot in range(2):
        xg_copy(0, 0, slot).wait()

        @pl.when(region == 0)
        def _(slot=slot):
            dy_copy(0, 0, slot).wait()


def gather_rows(tokens, slot_tok, slot_gate, cnt, nt, capacity):
    n_src = len(tokens)
    exp_local = cnt.shape[1]
    chunk = capacity // CHUNKS
    tok_dev = tokens[0].shape[0]
    width = SUB * LANES
    tile_rows = (n_src // 2) * chunk
    hbm = pl.BlockSpec(memory_space=pl.ANY)
    per_src = pl.BlockSpec((1, 1, exp_local * capacity), lambda s, *_: (s, 0, 0), memory_space=pltpu.SMEM)
    return pl.pallas_call(
        functools.partial(gather_kernel, n_src, exp_local, capacity, chunk),
        grid_spec=pltpu.PrefetchScalarGridSpec(
            num_scalar_prefetch=2,
            grid=(n_src,),
            in_specs=[per_src, per_src] + [hbm] * n_src,
            out_specs=[hbm, hbm],
            scratch_shapes=[
                pltpu.VMEM((tok_dev, SUB, LANES), jnp.bfloat16),
                pltpu.VMEM((chunk * SUB, LANES), jnp.float32),
                pltpu.VMEM((chunk * SUB, LANES), jnp.float32),
                pltpu.VMEM((2, chunk, width), jnp.bfloat16),
                pltpu.VMEM((2, chunk, width // 2), jnp.bfloat16),
                pltpu.SemaphoreType.DMA((2,)),
                pltpu.SemaphoreType.DMA((2,)),
                pltpu.SemaphoreType.DMA,
            ]),
        out_shape=[
            jax.ShapeDtypeStruct((exp_local, 2, CHUNKS, tile_rows, width), jnp.bfloat16),
            jax.ShapeDtypeStruct((exp_local, CHUNKS, tile_rows, width // 2), jnp.bfloat16),
        ],
        compiler_params=pltpu.CompilerParams(dimension_semantics=("arbitrary",)),
        name="gather_rows",
        interpret=INTERPRET,
    )(cnt.reshape(-1), nt.reshape(-1), slot_tok, slot_gate, *tokens)


def dot(a, b, dims):
    return lax.dot_general(a, b, (dims, ((), ())), preferred_element_type=jnp.float32)


NN, NT, TN = ((1,), (0,)), ((1,), (1,)), ((0,), (0,))


def expert_kernel(e0, step_rows, nt_ref, mine_ref, xg_ref, dy_ref, w1o, w1p, w3o, w3p, w2o, w2p, *refs):
    dx_ref, dr_ref, dw1_ref, dw3_ref, dw2_ref, h1, h3, da, hid, dh1, dh3, dw2t = refs[-12:]
    e = pl.program_id(0)
    t = pl.program_id(1)
    region, j = t // CHUNKS, t % CHUNKS
    half = w1o.shape[1]
    d_model = 2 * half
    mine = pl.multiple_of(mine_ref[0] * half, half)
    other = pl.multiple_of(half - mine_ref[0] * half, half)

    @pl.when(t == 0)
    def _():
        dw1_ref[...] = jnp.zeros_like(dw1_ref)
        dw3_ref[...] = jnp.zeros_like(dw3_ref)
        dw2t[...] = jnp.zeros_like(dw2t)

    @pl.when(j < nt_ref[(e0 + e) * 2 + region])
    def _():
        xo = xg_ref[0, 0, 0, :, pl.ds(mine, half)]
        xp = xg_ref[0, 0, 0, :, pl.ds(other, half)]
        go = xg_ref[0, 0, 0, :, pl.ds(d_model + mine, half)]
        gp = xg_ref[0, 0, 0, :, pl.ds(d_model + other, half)]
        h1[...] = dot(xo, w1o[0], NN) + dot(xp, w1p[0], NN)
        h3[...] = dot(xo, w3o[0], NN) + dot(xp, w3p[0], NN)
        da[...] = dot(go, w2o[0], NT) + dot(gp, w2p[0], NT)

        def rows(k, carry):
            at = pl.ds(pl.multiple_of(k * step_rows, step_rows), step_rows)
            p1, p3, d = h1[at, :], h3[at, :], da[at, :]
            s = jax.nn.sigmoid(p1)
            hid[at, :] = (p1 * s * p3).astype(jnp.bfloat16)
            dh1[at, :] = (d * p3 * s * (1.0 + p1 * (1.0 - s))).astype(jnp.bfloat16)
            dh3[at, :] = (d * p1 * s).astype(jnp.bfloat16)
            return carry

        lax.fori_loop(0, h1.shape[0] // step_rows, rows, 0)
        dw1_ref[0] += dot(xo, dh1[...], TN)
        dw3_ref[0] += dot(xo, dh3[...], TN)
        dw2t[...] += dot(go, hid[...], TN)

        @pl.when(region == 0)
        def _():
            dyo = dy_ref[0, 0, :, pl.ds(mine, half)].astype(jnp.float32)
            dyp = dy_ref[0, 0, :, pl.ds(other, half)].astype(jnp.float32)
            prod = dyo * dot(hid[...], w2o[0], NN) + dyp * dot(hid[...], w2p[0], NN)
            dr = jnp.sum(prod, axis=1, keepdims=True)
            lane = lax.broadcasted_iota(jnp.int32, dr_ref.shape[2:], 1)
            dr_ref[0, 0] = jnp.where(lane == e0 + e, dr, 0.0)
            dxo = dot(dh1[...], w1o[0], NT) + dot(dh3[...], w3o[0], NT)
            dx_ref[0, 0, :, pl.ds(mine, half)] = dxo.astype(jnp.bfloat16)
            dxp = dot(dh1[...], w1p[0], NT) + dot(dh3[...], w3p[0], NT)
            dx_ref[0, 0, :, pl.ds(other, half)] = dxp.astype(jnp.bfloat16)

    @pl.when(t == pl.num_programs(1) - 1)
    def _():
        dw2_ref[0] = dw2t[...].T


def expert_group(e0, count, xg, dy, nt, mine, own, peer, carried):
    exp_local, _, _, tile_rows, width = xg.shape
    half, d_ff = own[0].shape[1:]
    step_rows = 16

    def last(e, t, region, nt_ref):
        return jnp.minimum(jnp.where(t // CHUNKS == region, t % CHUNKS, CHUNKS - 1 if region == 0 else 0),
                           nt_ref[(e0 + e) * 2 + region] - 1)

    def xg_at(e, t, nt_ref, _):
        region = t // CHUNKS
        return (e0 + e, region, jnp.minimum(t % CHUNKS, nt_ref[(e0 + e) * 2 + region] - 1), 0, 0)

    def own_tile(e, t, nt_ref, _):
        return (e0 + e, last(e, t, 0, nt_ref), 0, 0)

    at_own = lambda e, t, *_: (e0 + e, 0, 0)
    at_peer = lambda e, t, *_: (e, 0, 0)
    up = lambda at: pl.BlockSpec((1, half, d_ff), at)
    down = lambda at: pl.BlockSpec((1, d_ff, half), at)
    out_shape = [
        jax.ShapeDtypeStruct((exp_local, CHUNKS, tile_rows, width // 2), jnp.bfloat16),
        jax.ShapeDtypeStruct((exp_local, CHUNKS, tile_rows, LANES), jnp.float32),
        jax.ShapeDtypeStruct((exp_local, half, d_ff), jnp.float32),
        jax.ShapeDtypeStruct((exp_local, half, d_ff), jnp.float32),
        jax.ShapeDtypeStruct((exp_local, d_ff, half), jnp.float32),
    ]
    n_in = 2 + 8
    carried = list(carried)
    return pl.pallas_call(
        functools.partial(expert_kernel, e0, step_rows),
        grid_spec=pltpu.PrefetchScalarGridSpec(
            num_scalar_prefetch=2,
            grid=(count, 2 * CHUNKS),
            in_specs=[
                pl.BlockSpec((1, 1, 1, tile_rows, width), xg_at),
                pl.BlockSpec((1, 1, tile_rows, width // 2), own_tile),
                up(at_own), up(at_peer), up(at_own), up(at_peer), down(at_own), down(at_peer),
            ] + [pl.BlockSpec(memory_space=pl.ANY)] * len(carried),
            out_specs=[
                pl.BlockSpec((1, 1, tile_rows, width // 2), own_tile),
                pl.BlockSpec((1, 1, tile_rows, LANES), own_tile),
                up(at_own), up(at_own), down(at_own),
            ],
            scratch_shapes=[
                pltpu.VMEM((tile_rows, d_ff), jnp.float32),
                pltpu.VMEM((tile_rows, d_ff), jnp.float32),
                pltpu.VMEM((tile_rows, d_ff), jnp.float32),
                pltpu.VMEM((tile_rows, d_ff), jnp.bfloat16),
                pltpu.VMEM((tile_rows, d_ff), jnp.bfloat16),
                pltpu.VMEM((tile_rows, d_ff), jnp.bfloat16),
                pltpu.VMEM((half, d_ff), jnp.float32),
            ]),
        out_shape=out_shape,
        input_output_aliases={n_in + k: k for k in range(len(carried))},
        compiler_params=pltpu.CompilerParams(
            dimension_semantics=("arbitrary", "arbitrary"), vmem_limit_bytes=60 * 1024 * 1024),
        name=f"experts_{e0}",
        interpret=INTERPRET,
    )(nt.reshape(-1), mine, xg, dy, own[0], peer[0], own[1], peer[1], own[2], peer[2], *carried)


def scatter_kernel(exp_local, capacity, chunk, cnt_ref, nt_ref, tok_ref, dx_hbm, dr_hbm,
                   dx_out, dr_out, acc, tmp, dx_v, dr_v, dx_sem, dr_sem):
    src = pl.program_id(0)

    def copies(e, j):
        k = e * CHUNKS + j
        rows = pl.ds(src * chunk, chunk)
        return (pltpu.make_async_copy(dx_hbm.at[e, j, rows], dx_v.at[k], dx_sem.at[k]),
                pltpu.make_async_copy(dr_hbm.at[e, j, rows], dr_v.at[k], dr_sem.at[k]))

    def each(fn):
        def per_expert(e, carry):
            n = cnt_ref[src * exp_local + e]
            lax.fori_loop(0, (n + chunk - 1) // chunk, lambda j, c: fn(e, j, n, c), 0)
            return carry
        lax.fori_loop(0, exp_local, per_expert, 0)

    def start(e, j, n, carry):
        for copy in copies(e, j):
            copy.start()
        return carry

    each(start)
    acc[...] = jnp.zeros_like(acc)

    def add(e, j, n, carry):
        k = e * CHUNKS + j
        for copy in copies(e, j):
            copy.wait()
        for c in range(SUB // 2):
            tmp[pl.ds(c, chunk, stride=SUB), :] = dx_v[k, :, c * LANES:(c + 1) * LANES].astype(jnp.float32)
        tmp[pl.ds(SUB // 2, chunk, stride=SUB), :] = dr_v[k]

        def row(r, c):
            t = tok_ref[0, 0, e * capacity + j * chunk + r]
            at = pl.ds(pl.multiple_of(t * SUB, SUB), SUB)
            acc[at, :] += tmp[pl.ds(pl.multiple_of(r * SUB, SUB), SUB), :]
            return c

        lax.fori_loop(0, jnp.minimum(n - j * chunk, chunk), row, 0)
        return carry

    each(add)
    tok_dev = dx_out.shape[1]
    for c in range(SUB // 2):
        dx_out[0, :, c * LANES:(c + 1) * LANES] = acc[pl.ds(c, tok_dev, stride=SUB), :]
    dr_out[0] = acc[pl.ds(SUB // 2, tok_dev, stride=SUB), :]


def scatter_rows(dx_rows, dr_rows, slot_tok, cnt, nt, capacity, tok_dev):
    exp_local, _, tile_rows, d_model = dx_rows.shape
    chunk = capacity // CHUNKS
    n_own = tile_rows // chunk
    hbm = pl.BlockSpec(memory_space=pl.ANY)
    return pl.pallas_call(
        functools.partial(scatter_kernel, exp_local, capacity, chunk),
        grid_spec=pltpu.PrefetchScalarGridSpec(
            num_scalar_prefetch=2,
            grid=(n_own,),
            in_specs=[
                pl.BlockSpec((1, 1, exp_local * capacity), lambda s, *_: (s, 0, 0), memory_space=pltpu.SMEM),
                hbm, hbm,
            ],
            out_specs=[
                pl.BlockSpec((1, tok_dev, d_model), lambda s, *_: (s, 0, 0)),
                pl.BlockSpec((1, tok_dev, LANES), lambda s, *_: (s, 0, 0)),
            ],
            scratch_shapes=[
                pltpu.VMEM((tok_dev * SUB, LANES), jnp.float32),
                pltpu.VMEM((chunk * SUB, LANES), jnp.float32),
                pltpu.VMEM((exp_local * CHUNKS, chunk, d_model), jnp.bfloat16),
                pltpu.VMEM((exp_local * CHUNKS, chunk, LANES), jnp.float32),
                pltpu.SemaphoreType.DMA((exp_local * CHUNKS,)),
                pltpu.SemaphoreType.DMA((exp_local * CHUNKS,)),
            ]),
        out_shape=[
            jax.ShapeDtypeStruct((n_own, tok_dev, d_model), jnp.float32),
            jax.ShapeDtypeStruct((n_own, tok_dev, LANES), jnp.float32),
        ],
        compiler_params=pltpu.CompilerParams(
            dimension_semantics=("arbitrary",), vmem_limit_bytes=60 * 1024 * 1024),
        name="scatter_rows",
        interpret=INTERPRET,
    )(cnt.reshape(-1), nt.reshape(-1), slot_tok, dx_rows, dr_rows)


def solution(mesh):
    n_ep = mesh.shape["ep"]
    n_fsdp = mesh.shape["fsdp"]
    tok_spec = P(("fsdp", "ep"), None)
    spec_in = P("ep", "fsdp", None)
    spec_out = P("ep", None, "fsdp")

    def swap(value, axis, mask):
        size = n_fsdp if axis == "fsdp" else n_ep
        return lax.ppermute(value, axis, [(k, k ^ mask) for k in range(size)])

    def per_device(x_tok, dy_tok, expert_ids, route_w, w_gate, w_up, w_down):
        tok_dev, top_k = expert_ids.shape
        exp_local = w_gate.shape[0]
        experts = exp_local * n_ep
        capacity = capacity_of(tok_dev, top_k, experts)
        chunk = capacity // CHUNKS
        my_fsdp = lax.axis_index("fsdp")
        my_ep = lax.axis_index("ep")

        tokens = jnp.concatenate([x_tok, dy_tok], axis=1).reshape(tok_dev, SUB, LANES)
        tok_y = swap(tokens, "fsdp", 1)
        tok_x = swap(tokens, "ep", 2)
        tok_c = swap(tokens, "ep", 1)
        tok_yx = swap(tok_y, "ep", 2)
        tok_cx = swap(tok_x, "ep", 1)
        tok_cy = swap(tok_y, "ep", 1)
        tok_cyx = swap(tok_yx, "ep", 1)
        all_tokens = (tokens, tok_c, tok_x, tok_cx, tok_y, tok_cy, tok_yx, tok_cyx)

        own = (w_gate, w_up, w_down)
        peers = []
        e0 = 0
        gate = tok_y
        for g, count in enumerate(GROUPS):
            part = [w[e0:e0 + count] for w in own]
            if g >= 2:
                gate = peers[g - 2][2]
            *part, _ = lax.optimization_barrier((*part, gate))
            peers.append([swap(w, "fsdp", 1) for w in part])
            e0 += count

        slot_tok, slot_gate, cnt = route_slots(expert_ids.reshape(-1), route_w.reshape(-1), top_k, experts, capacity)

        def from_all(v):
            v = lax.all_gather(v, ("fsdp", "ep"), axis=0, tiled=False)
            v = v.reshape(n_fsdp * n_ep, n_ep, -1)
            v = lax.dynamic_index_in_dim(v, my_ep, axis=1, keepdims=False)
            order = [(my_fsdp ^ a) * n_ep + (my_ep ^ b) for a in range(n_fsdp) for b in range(n_ep)]
            return jnp.stack([lax.dynamic_index_in_dim(v, k, axis=0, keepdims=False) for k in order])

        slot_tok, slot_gate, cnt = from_all(slot_tok), from_all(slot_gate), from_all(cnt)
        n_src = n_fsdp * n_ep
        slot_tok = slot_tok.reshape(n_src, 1, -1)
        slot_gate = slot_gate.reshape(n_src, 1, -1)
        most = jnp.max(cnt.reshape(n_fsdp, n_ep, exp_local), axis=1)
        nt = jnp.maximum((most + chunk - 1) // chunk, 1).T

        xg, dy = gather_rows(all_tokens, slot_tok, slot_gate, cnt, nt, capacity)
        mine = my_fsdp.astype(jnp.int32).reshape(1)
        carried = ()
        e0 = 0
        for count, peer in zip(GROUPS, peers):
            carried = expert_group(e0, count, xg, dy, nt, mine, own, peer, carried)
            e0 += count
        dx_rows, dr_rows, grad_w_gate, grad_w_up, grad_w_down = carried

        part, dr_part = scatter_rows(dx_rows, dr_rows, slot_tok[:n_ep], cnt[:n_ep], nt, capacity, tok_dev)
        from_core_near = swap(part[1], "ep", 1)
        from_core_far = swap(part[3], "ep", 1)
        far = part[2] + from_core_far
        near = part[0] + from_core_near
        grad_x = (near + swap(far, "ep", 2)).astype(jnp.bfloat16)
        dr_mine = dr_part[:, :, :exp_local]
        by_ep = jnp.stack([dr_mine[0]] + [swap(dr_mine[b], "ep", b) for b in range(1, n_ep)])
        rel = (expert_ids // exp_local) ^ my_ep
        loc = expert_ids % exp_local
        hit = ((rel[:, :, None, None] == jnp.arange(n_ep)[None, None, :, None])
               & (loc[:, :, None, None] == jnp.arange(exp_local)[None, None, None, :]))
        dense = jnp.transpose(by_ep, (1, 0, 2))[:, None]
        route_grad = jnp.sum(jnp.where(hit, dense, 0.0), axis=(2, 3))
        return grad_x, route_grad, grad_w_gate, grad_w_up, grad_w_down

    return jax.shard_map(
        per_device, mesh=mesh,
        in_specs=(tok_spec, tok_spec, tok_spec, tok_spec, spec_in, spec_in, spec_out),
        out_specs=(tok_spec, tok_spec, spec_in, spec_in, spec_out),
        check_vma=False)
```

```python
import functools

import jax
import jax.numpy as jnp
from jax import lax
from jax.experimental import pallas as pl
from jax.experimental.pallas import tpu as pltpu
from jax.sharding import PartitionSpec as P


CAP_FACTOR = 3
CHUNKS = 4
GROUPS = (3, 3, 3, 3, 2, 2)
PAD = 8
LANES = 128
SUB = 8
INTERPRET = False
VMEM_BYTES = 67_043_328


def capacity_of(tok_dev, top_k, experts):
    return max(8, ((CAP_FACTOR * tok_dev * top_k // experts + 7) // 8) * 8)


def route_kernel(n_pairs, top_k, experts, capacity, ids_ref, gate_ref, tok_ref, slot_gate_ref, cnt_ref):
    stride = capacity + PAD
    for e in range(experts):
        cnt_ref[e] = 0

    def step(t, carry):
        ids = [ids_ref[t * top_k + j] for j in range(top_k)]
        gates = [gate_ref[t * top_k + j] for j in range(top_k)]
        counts = [cnt_ref[e] for e in ids]
        for j in range(top_k):
            slot = ids[j] * stride + jnp.minimum(counts[j], capacity)
            tok_ref[slot] = t
            slot_gate_ref[slot] = gates[j]
            cnt_ref[ids[j]] = counts[j] + 1
        return carry

    lax.fori_loop(0, n_pairs // top_k, step, 0, unroll=2)
    for e in range(experts):
        tok_ref[e * stride + capacity + 1] = jnp.minimum(cnt_ref[e], capacity)


def route_slots(ids_flat, gates_flat, top_k, experts, capacity):
    n_pairs = ids_flat.shape[0]
    smem = pl.BlockSpec(memory_space=pltpu.SMEM)
    words = experts * (capacity + PAD)
    return pl.pallas_call(
        functools.partial(route_kernel, n_pairs, top_k, experts, capacity),
        in_specs=[smem, smem],
        out_specs=[smem, smem],
        out_shape=[jax.ShapeDtypeStruct((words,), jnp.int32), jax.ShapeDtypeStruct((words,), jnp.float32)],
        scratch_shapes=[pltpu.SMEM((experts,), jnp.int32)],
        name="route",
        interpret=INTERPRET,
    )(ids_flat, gates_flat)


def gather_kernel(n_src, with_dy, region, exp_local, capacity, chunk, nt_ref, tok_ref, gate_ref, *refs):
    stride = capacity + PAD
    token_refs = refs[:n_src]
    refs = list(refs[n_src if with_dy else n_src + 1:])
    xg_hbm = refs.pop(0)
    dy_hbm = refs.pop(0) if with_dy else None
    rows_v, buf_x, buf_g, xg_v, dy_v, xg_sem, dy_sem, tok_sem = refs
    src = pl.program_id(0)
    for k in range(n_src):
        @pl.when(src == k)
        def _(k=k):
            copy = pltpu.make_async_copy(token_refs[k], rows_v, tok_sem)
            copy.start()
            copy.wait()

    def copies(e, j, slot):
        at = pl.ds(src * chunk, chunk)
        out = [pltpu.make_async_copy(xg_v.at[slot], xg_hbm.at[e, region, j, at], xg_sem.at[slot])]
        if with_dy:
            out.append(pltpu.make_async_copy(dy_v.at[slot], dy_hbm.at[e, j, at], dy_sem.at[slot]))
        return out

    def one_expert(e, done):
        n = tok_ref[0, 0, e * stride + capacity + 1]

        def one_chunk(j, done):
            slot = lax.rem(done, 2)

            @pl.when(done >= 2)
            def _():
                for copy in copies(e, j, slot):
                    copy.wait()

            def rows(r8, carry):
                at0 = j * chunk + r8 * 8
                toks = [jnp.where(at0 + u < n, tok_ref[0, 0, e * stride + at0 + u], 0) for u in range(8)]
                gates = [jnp.where(at0 + u < n, gate_ref[0, 0, e * stride + at0 + u], 0.0) for u in range(8)]
                loaded = [rows_v[t].astype(jnp.float32) for t in toks]
                for u in range(8):
                    at = pl.ds(pl.multiple_of((r8 * 8 + u) * SUB, SUB), SUB)
                    buf_x[at, :] = loaded[u]
                    buf_g[at, :] = loaded[u] * gates[u]
                return carry

            lax.fori_loop(0, chunk // 8, rows, 0)
            half = SUB // 2
            for c in range(half):
                lanes = slice(c * LANES, (c + 1) * LANES)
                g_lanes = slice((half + c) * LANES, (half + c + 1) * LANES)
                xg_v[slot, :, lanes] = buf_x[pl.ds(c, chunk, stride=SUB), :].astype(jnp.bfloat16)
                xg_v[slot, :, g_lanes] = buf_g[pl.ds(half + c, chunk, stride=SUB), :].astype(jnp.bfloat16)
                if with_dy:
                    dy_v[slot, :, lanes] = buf_x[pl.ds(half + c, chunk, stride=SUB), :].astype(jnp.bfloat16)
            for copy in copies(e, j, slot):
                copy.start()
            return done + 1

        return lax.fori_loop(0, nt_ref[e * 2 + region], one_chunk, done)

    lax.fori_loop(0, exp_local, one_expert, 0)
    for slot in range(2):
        for copy in copies(0, 0, slot):
            copy.wait()


def gather_rows(tokens, slot_tok, slot_gate, nt, region, capacity, carried=()):
    with_dy = region == 0
    n_src = len(tokens)
    exp_local = nt.shape[0]
    chunk = capacity // CHUNKS
    tok_dev = tokens[0].shape[0]
    width = SUB * LANES
    tile_rows = n_src * chunk
    hbm = pl.BlockSpec(memory_space=pl.ANY)
    per_src = pl.BlockSpec((1, 1, slot_tok.shape[2]), lambda s, *_: (s, 0, 0), memory_space=pltpu.SMEM)
    out_shape = [jax.ShapeDtypeStruct((exp_local, 2, CHUNKS, tile_rows, width), jnp.bfloat16)]
    if with_dy:
        out_shape.append(jax.ShapeDtypeStruct((exp_local, CHUNKS, tile_rows, width // 2), jnp.bfloat16))
    return pl.pallas_call(
        functools.partial(gather_kernel, n_src, with_dy, region, exp_local, capacity, chunk),
        grid_spec=pltpu.PrefetchScalarGridSpec(
            num_scalar_prefetch=1,
            grid=(n_src,),
            in_specs=[per_src, per_src] + [hbm] * (n_src + len(carried)),
            out_specs=[hbm] * len(out_shape),
            scratch_shapes=[
                pltpu.VMEM((tok_dev, SUB, LANES), jnp.bfloat16),
                pltpu.VMEM((chunk * SUB, LANES), jnp.float32),
                pltpu.VMEM((chunk * SUB, LANES), jnp.float32),
                pltpu.VMEM((2, chunk, width), jnp.bfloat16),
                pltpu.VMEM((2, chunk, width // 2), jnp.bfloat16),
                pltpu.SemaphoreType.DMA((2,)),
                pltpu.SemaphoreType.DMA((2,)),
                pltpu.SemaphoreType.DMA,
            ]),
        out_shape=out_shape,
        input_output_aliases={3 + n_src + k: k for k in range(len(carried))},
        compiler_params=pltpu.CompilerParams(dimension_semantics=("arbitrary",), vmem_limit_bytes=VMEM_BYTES),
        interpret=INTERPRET,
    )(nt.reshape(-1), slot_tok, slot_gate, *tokens, *carried)


def dot(a, b, dims):
    return lax.dot_general(a, b, (dims, ((), ())), preferred_element_type=jnp.float32)


NN, NT, TN = ((1,), (0,)), ((1,), (1,)), ((0,), (0,))


def expert_kernel(e0, step_rows, nt_ref, mine_ref, xg_ref, dy_ref, w1o, w1p, w3o, w3p, w2o, w2p, *refs):
    dx_ref, dr_ref, dw1_ref, dw3_ref, dw2_ref, h1, h3, da, hid, dh1, dh3, dw2t = refs[-12:]
    e = pl.program_id(0)
    t = pl.program_id(1)
    region, j = t // CHUNKS, t % CHUNKS
    half = w1o.shape[1]
    d_model = 2 * half
    mine = pl.multiple_of(mine_ref[0] * half, half)
    other = pl.multiple_of(half - mine_ref[0] * half, half)

    @pl.when(t == 0)
    def _():
        dw1_ref[...] = jnp.zeros_like(dw1_ref)
        dw3_ref[...] = jnp.zeros_like(dw3_ref)
        dw2t[...] = jnp.zeros_like(dw2t)

    @pl.when(j < nt_ref[(e0 + e) * 2 + region])
    def _():
        xo = xg_ref[0, 0, 0, :, pl.ds(mine, half)]
        xp = xg_ref[0, 0, 0, :, pl.ds(other, half)]
        go = xg_ref[0, 0, 0, :, pl.ds(d_model + mine, half)]
        gp = xg_ref[0, 0, 0, :, pl.ds(d_model + other, half)]
        h1[...] = dot(xo, w1o[0], NN) + dot(xp, w1p[0], NN)
        h3[...] = dot(xo, w3o[0], NN) + dot(xp, w3p[0], NN)
        da[...] = dot(go, w2o[0], NT) + dot(gp, w2p[0], NT)

        def rows(k, carry):
            at = pl.ds(pl.multiple_of(k * step_rows, step_rows), step_rows)
            p1, p3, d = h1[at, :], h3[at, :], da[at, :]
            s = jax.nn.sigmoid(p1)
            hid[at, :] = (p1 * s * p3).astype(jnp.bfloat16)
            dh1[at, :] = (d * p3 * s * (1.0 + p1 * (1.0 - s))).astype(jnp.bfloat16)
            dh3[at, :] = (d * p1 * s).astype(jnp.bfloat16)
            return carry

        lax.fori_loop(0, h1.shape[0] // step_rows, rows, 0)
        dw1_ref[0] += dot(xo, dh1[...], TN)
        dw3_ref[0] += dot(xo, dh3[...], TN)
        dw2t[...] += dot(go, hid[...], TN)

    @pl.when((region == 0) & (j < nt_ref[(e0 + e) * 2]))
    def _():
        dyo = dy_ref[0, 0, :, pl.ds(mine, half)].astype(jnp.float32)
        dyp = dy_ref[0, 0, :, pl.ds(other, half)].astype(jnp.float32)
        prod = dyo * dot(hid[...], w2o[0], NN) + dyp * dot(hid[...], w2p[0], NN)
        dr = jnp.sum(prod, axis=1, keepdims=True)
        lane = lax.broadcasted_iota(jnp.int32, dr_ref.shape[2:], 1)
        dr_ref[0, 0] = jnp.where(lane == e0 + e, dr, 0.0)
        dxo = dot(dh1[...], w1o[0], NT) + dot(dh3[...], w3o[0], NT)
        dx_ref[0, 0, :, pl.ds(mine, half)] = dxo.astype(jnp.bfloat16)
        dxp = dot(dh1[...], w1p[0], NT) + dot(dh3[...], w3p[0], NT)
        dx_ref[0, 0, :, pl.ds(other, half)] = dxp.astype(jnp.bfloat16)

    @pl.when(t == pl.num_programs(1) - 1)
    def _():
        dw2_ref[0] = dw2t[...].T


def expert_group(e0, count, xg, dy, nt, mine, own, peer, carried):
    exp_local, _, _, tile_rows, width = xg.shape
    half, d_ff = own[0].shape[1:]
    step_rows = 16

    def own_tile(e, t, nt_ref, _):
        return (e0 + e, jnp.minimum(jnp.where(t < CHUNKS, t, CHUNKS - 1), nt_ref[(e0 + e) * 2] - 1), 0, 0)

    def xg_tile(e, t, nt_ref, _):
        region = t // CHUNKS
        return (e0 + e, region, jnp.minimum(t % CHUNKS, nt_ref[(e0 + e) * 2 + region] - 1), 0, 0)

    at_own = lambda e, t, *_: (e0 + e, 0, 0)
    at_peer = lambda e, t, *_: (e, 0, 0)
    up = lambda at: pl.BlockSpec((1, half, d_ff), at)
    down = lambda at: pl.BlockSpec((1, d_ff, half), at)
    out_shape = [
        jax.ShapeDtypeStruct((exp_local, CHUNKS, tile_rows, width // 2), jnp.bfloat16),
        jax.ShapeDtypeStruct((exp_local, CHUNKS, tile_rows, LANES), jnp.float32),
        jax.ShapeDtypeStruct((exp_local, half, d_ff), jnp.float32),
        jax.ShapeDtypeStruct((exp_local, half, d_ff), jnp.float32),
        jax.ShapeDtypeStruct((exp_local, d_ff, half), jnp.float32),
    ]
    n_in = 2 + 8
    carried = list(carried)
    return pl.pallas_call(
        functools.partial(expert_kernel, e0, step_rows),
        grid_spec=pltpu.PrefetchScalarGridSpec(
            num_scalar_prefetch=2,
            grid=(count, 2 * CHUNKS),
            in_specs=[
                pl.BlockSpec((1, 1, 1, tile_rows, width), xg_tile),
                pl.BlockSpec((1, 1, tile_rows, width // 2), own_tile),
                up(at_own), up(at_peer), up(at_own), up(at_peer), down(at_own), down(at_peer),
            ] + [pl.BlockSpec(memory_space=pl.ANY)] * len(carried),
            out_specs=[
                pl.BlockSpec((1, 1, tile_rows, width // 2), own_tile),
                pl.BlockSpec((1, 1, tile_rows, LANES), own_tile),
                up(at_own), up(at_own), down(at_own),
            ],
            scratch_shapes=[
                pltpu.VMEM((tile_rows, d_ff), jnp.float32),
                pltpu.VMEM((tile_rows, d_ff), jnp.float32),
                pltpu.VMEM((tile_rows, d_ff), jnp.float32),
                pltpu.VMEM((tile_rows, d_ff), jnp.bfloat16),
                pltpu.VMEM((tile_rows, d_ff), jnp.bfloat16),
                pltpu.VMEM((tile_rows, d_ff), jnp.bfloat16),
                pltpu.VMEM((half, d_ff), jnp.float32),
            ]),
        out_shape=out_shape,
        input_output_aliases={n_in + k: k for k in range(len(carried))},
        compiler_params=pltpu.CompilerParams(
            dimension_semantics=("arbitrary", "arbitrary"), vmem_limit_bytes=VMEM_BYTES),
        interpret=INTERPRET,
    )(nt.reshape(-1), mine, xg, dy, own[0], peer[0], own[1], peer[1], own[2], peer[2], *carried)


def scatter_kernel(exp_local, capacity, chunk, tok_ref, dx_hbm, dr_hbm,
                   dx_out, dr_out, acc, tmp, dx_v, dr_v, dx_sem, dr_sem):
    src = pl.program_id(0)
    stride = capacity + PAD
    tok_dev = dx_out.shape[1]

    def copies(e, j):
        k = e * CHUNKS + j
        rows = pl.ds(src * chunk, chunk)
        return (pltpu.make_async_copy(dx_hbm.at[e, j, rows], dx_v.at[k], dx_sem.at[k]),
                pltpu.make_async_copy(dr_hbm.at[e, j, rows], dr_v.at[k], dr_sem.at[k]))

    def each(fn):
        def per_expert(e, carry):
            n = tok_ref[0, 0, e * stride + capacity + 1]
            lax.fori_loop(0, (n + chunk - 1) // chunk, lambda j, c: fn(e, j, n, c), 0)
            return carry

        lax.fori_loop(0, exp_local, per_expert, 0)

    def start(e, j, n, carry):
        for copy in copies(e, j):
            copy.start()
        return carry

    each(start)
    acc[...] = jnp.zeros_like(acc)

    def add(e, j, n, carry):
        k = e * CHUNKS + j
        for copy in copies(e, j):
            copy.wait()
        for c in range(SUB // 2):
            tmp[pl.ds(c, chunk, stride=SUB), :] = dx_v[k, :, c * LANES:(c + 1) * LANES].astype(jnp.float32)
        tmp[pl.ds(SUB // 2, chunk, stride=SUB), :] = dr_v[k]

        def rows(r8, c):
            r0 = r8 * 8
            toks = [jnp.where(j * chunk + r0 + u < n, tok_ref[0, 0, e * stride + j * chunk + r0 + u], tok_dev)
                    for u in range(8)]
            ats = [pl.ds(pl.multiple_of(t * SUB, SUB), SUB) for t in toks]
            sums = [acc[ats[u], :] + tmp[pl.ds(pl.multiple_of((r0 + u) * SUB, SUB), SUB), :] for u in range(8)]
            for u in range(8):
                acc[ats[u], :] = sums[u]
            return c

        lax.fori_loop(0, (jnp.minimum(n - j * chunk, chunk) + 7) // 8, rows, 0)
        return carry

    each(add)
    for c in range(SUB // 2):
        dx_out[0, :, c * LANES:(c + 1) * LANES] = acc[pl.ds(c, tok_dev, stride=SUB), :]
    dr_out[0] = acc[pl.ds(SUB // 2, tok_dev, stride=SUB), :]


def scatter_rows(dx_rows, dr_rows, slot_tok, capacity, tok_dev):
    exp_local, _, tile_rows, d_model = dx_rows.shape
    chunk = capacity // CHUNKS
    n_own = tile_rows // chunk
    hbm = pl.BlockSpec(memory_space=pl.ANY)
    return pl.pallas_call(
        functools.partial(scatter_kernel, exp_local, capacity, chunk),
        grid_spec=pltpu.PrefetchScalarGridSpec(
            num_scalar_prefetch=0,
            grid=(n_own,),
            in_specs=[
                pl.BlockSpec((1, 1, slot_tok.shape[2]), lambda s, *_: (s, 0, 0), memory_space=pltpu.SMEM),
                hbm, hbm,
            ],
            out_specs=[
                pl.BlockSpec((1, tok_dev, d_model), lambda s, *_: (s, 0, 0)),
                pl.BlockSpec((1, tok_dev, LANES), lambda s, *_: (s, 0, 0)),
            ],
            scratch_shapes=[
                pltpu.VMEM(((tok_dev + 1) * SUB, LANES), jnp.float32),
                pltpu.VMEM((chunk * SUB, LANES), jnp.float32),
                pltpu.VMEM((exp_local * CHUNKS, chunk, d_model), jnp.bfloat16),
                pltpu.VMEM((exp_local * CHUNKS, chunk, LANES), jnp.float32),
                pltpu.SemaphoreType.DMA((exp_local * CHUNKS,)),
                pltpu.SemaphoreType.DMA((exp_local * CHUNKS,)),
            ]),
        out_shape=[
            jax.ShapeDtypeStruct((n_own, tok_dev, d_model), jnp.float32),
            jax.ShapeDtypeStruct((n_own, tok_dev, LANES), jnp.float32),
        ],
        compiler_params=pltpu.CompilerParams(
            dimension_semantics=("arbitrary",), vmem_limit_bytes=VMEM_BYTES),
        name="scatter_rows",
        interpret=INTERPRET,
    )(slot_tok, dx_rows, dr_rows)


def solution(mesh):
    n_ep = mesh.shape["ep"]
    n_fsdp = mesh.shape["fsdp"]
    tok_spec = P(("fsdp", "ep"), None)
    spec_in = P("ep", "fsdp", None)
    spec_out = P("ep", None, "fsdp")

    def swap(value, axis, mask):
        size = n_fsdp if axis == "fsdp" else n_ep
        return lax.ppermute(value, axis, [(k, k ^ mask) for k in range(size)])

    def per_device(x_tok, dy_tok, expert_ids, route_w, w_gate, w_up, w_down):
        tok_dev, top_k = expert_ids.shape
        exp_local = w_gate.shape[0]
        experts = exp_local * n_ep
        capacity = capacity_of(tok_dev, top_k, experts)
        chunk = capacity // CHUNKS
        my_fsdp = lax.axis_index("fsdp")
        my_ep = lax.axis_index("ep")

        tokens = jnp.concatenate([x_tok, dy_tok], axis=1).reshape(tok_dev, SUB, LANES)
        tok_y = swap(tokens, "fsdp", 1)
        tok_x = swap(tokens, "ep", 2)
        tok_c = swap(tokens, "ep", 1)
        tok_yx = swap(tok_y, "ep", 2)
        tok_cx = swap(tok_x, "ep", 1)
        tok_cy = swap(tok_y, "ep", 1)
        tok_cyx = swap(tok_yx, "ep", 1)
        all_tokens = (tokens, tok_c, tok_x, tok_cx, tok_y, tok_cy, tok_yx, tok_cyx)

        slot_tok, slot_gate = route_slots(
            expert_ids.reshape(-1), route_w.reshape(-1), top_k, experts, capacity)
        slot_tok = lax.all_gather(slot_tok, ("fsdp", "ep"), axis=0, tiled=False)
        slot_gate = lax.all_gather(slot_gate, ("fsdp", "ep"), axis=0, tiled=False)

        def for_me(v):
            v = v.reshape(n_fsdp * n_ep, n_ep, -1)
            v = lax.dynamic_index_in_dim(v, my_ep, axis=1, keepdims=False)
            order = [(my_fsdp ^ a) * n_ep + (my_ep ^ b) for a in range(n_fsdp) for b in range(n_ep)]
            return jnp.stack([lax.dynamic_index_in_dim(v, k, axis=0, keepdims=True) for k in order])

        slot_tok, slot_gate = for_me(slot_tok), for_me(slot_gate)
        cnt = slot_tok.reshape(n_fsdp, n_ep, exp_local, capacity + PAD)[..., capacity + 1]
        most = jnp.max(cnt, axis=1)
        nt = jnp.maximum((most + chunk - 1) // chunk, 1).T

        xg, dy = gather_rows(all_tokens[:n_ep], slot_tok[:n_ep], slot_gate[:n_ep], nt, 0, capacity)
        xg, = gather_rows(all_tokens[n_ep:], slot_tok[n_ep:], slot_gate[n_ep:], nt, 1, capacity, (xg,))

        own = (w_gate, w_up, w_down)
        mine = my_fsdp.astype(jnp.int32).reshape(1)
        carried = ()
        e0 = 0
        for count in GROUPS:
            peer = [swap(w[e0:e0 + count], "fsdp", 1) for w in own]
            carried = expert_group(e0, count, xg, dy, nt, mine, own, peer, carried)
            e0 += count
        dx_rows, dr_rows, grad_w_gate, grad_w_up, grad_w_down = carried

        part, dr_part = scatter_rows(dx_rows, dr_rows, slot_tok[:n_ep], capacity, tok_dev)
        from_core_near = swap(part[1], "ep", 1)
        from_core_far = swap(part[3], "ep", 1)
        far = part[2] + from_core_far
        near = part[0] + from_core_near
        grad_x = (near + swap(far, "ep", 2)).astype(jnp.bfloat16)
        dr_mine = dr_part[:, :, :exp_local]
        by_ep = jnp.stack([dr_mine[0]] + [swap(dr_mine[b], "ep", b) for b in range(1, n_ep)])
        rel = (expert_ids // exp_local) ^ my_ep
        loc = expert_ids % exp_local
        hit = ((rel[:, :, None, None] == jnp.arange(n_ep)[None, None, :, None])
               & (loc[:, :, None, None] == jnp.arange(exp_local)[None, None, None, :]))
        dense = jnp.transpose(by_ep, (1, 0, 2))[:, None]
        route_grad = jnp.sum(jnp.where(hit, dense, 0.0), axis=(2, 3))
        return grad_x, route_grad, grad_w_gate, grad_w_up, grad_w_down

    return jax.shard_map(
        per_device, mesh=mesh,
        in_specs=(tok_spec, tok_spec, tok_spec, tok_spec, spec_in, spec_in, spec_out),
        out_specs=(tok_spec, tok_spec, spec_in, spec_in, spec_out),
        check_vma=False)
```

```python
import functools

import jax
import jax.numpy as jnp
from jax import lax
from jax.experimental import pallas as pl
from jax.experimental.pallas import tpu as pltpu
from jax.sharding import PartitionSpec as P


CAP_FACTOR = 3
CHUNKS = 4
GROUPS = (4, 4, 2, 2, 2, 1, 1)
STAGES = ((0, 1), (2, 3, 4, 5, 6))
PAD = 8
LANES = 128
N_OWN = 4
SUB = 8
INTERPRET = False
VMEM_BYTES = 67_043_328


def capacity_of(tok_dev, top_k, experts):
    return max(8, ((CAP_FACTOR * tok_dev * top_k // experts + 7) // 8) * 8)


def route_kernel(n_pairs, top_k, experts, capacity, ids_ref, gate_ref, tok_ref, slot_gate_ref, cnt_ref):
    stride = capacity + PAD
    for e in range(experts):
        cnt_ref[e] = 0

    def step(t, carry):
        ids = [ids_ref[t * top_k + j] for j in range(top_k)]
        gates = [gate_ref[t * top_k + j] for j in range(top_k)]
        counts = [cnt_ref[e] for e in ids]
        for j in range(top_k):
            slot = ids[j] * stride + jnp.minimum(counts[j], capacity)
            tok_ref[slot] = t
            slot_gate_ref[slot] = gates[j]
            cnt_ref[ids[j]] = counts[j] + 1
        return carry

    lax.fori_loop(0, n_pairs // top_k, step, 0, unroll=2)
    for e in range(experts):
        tok_ref[e * stride + capacity + 1] = jnp.minimum(cnt_ref[e], capacity)


def route_slots(ids_flat, gates_flat, top_k, experts, capacity):
    n_pairs = ids_flat.shape[0]
    smem = pl.BlockSpec(memory_space=pltpu.SMEM)
    words = experts * (capacity + PAD)
    return pl.pallas_call(
        functools.partial(route_kernel, n_pairs, top_k, experts, capacity),
        in_specs=[smem, smem],
        out_specs=[smem, smem],
        out_shape=[jax.ShapeDtypeStruct((words,), jnp.int32), jax.ShapeDtypeStruct((words,), jnp.float32)],
        scratch_shapes=[pltpu.SMEM((experts,), jnp.int32)],
        name="route",
        interpret=INTERPRET,
    )(ids_flat, gates_flat)


def gather_kernel(n_src, with_dy, region, exp_local, capacity, chunk, nt_ref, tok_ref, gate_ref, *refs):
    stride = capacity + PAD
    token_refs = refs[:n_src]
    refs = list(refs[n_src if with_dy else n_src + 1:])
    xg_hbm = refs.pop(0)
    dy_hbm = refs.pop(0) if with_dy else None
    rows_v, buf_x, buf_g, xg_v, dy_v, xg_sem, dy_sem, tok_sem = refs
    src = pl.program_id(0)
    for k in range(n_src):
        @pl.when(src == k)
        def _(k=k):
            copy = pltpu.make_async_copy(token_refs[k], rows_v, tok_sem)
            copy.start()
            copy.wait()

    def copies(e, j, slot):
        at = pl.ds(src * chunk, chunk)
        out = [pltpu.make_async_copy(xg_v.at[slot], xg_hbm.at[e, region, j, at], xg_sem.at[slot])]
        if with_dy:
            out.append(pltpu.make_async_copy(dy_v.at[slot], dy_hbm.at[e, j, at], dy_sem.at[slot]))
        return out

    def one_expert(e, done):
        n = tok_ref[0, 0, e * stride + capacity + 1]

        def one_chunk(j, done):
            slot = lax.rem(done, 2)

            @pl.when(done >= 2)
            def _():
                for copy in copies(e, j, slot):
                    copy.wait()

            def rows(r8, carry):
                at0 = j * chunk + r8 * 8
                toks = [jnp.where(at0 + u < n, tok_ref[0, 0, e * stride + at0 + u], 0) for u in range(8)]
                gates = [jnp.where(at0 + u < n, gate_ref[0, 0, e * stride + at0 + u], 0.0) for u in range(8)]
                loaded = [rows_v[t].astype(jnp.float32) for t in toks]
                for u in range(8):
                    at = pl.ds(pl.multiple_of((r8 * 8 + u) * SUB, SUB), SUB)
                    buf_x[at, :] = loaded[u]
                    buf_g[at, :] = loaded[u] * gates[u]
                return carry

            lax.fori_loop(0, chunk // 8, rows, 0)
            half = SUB // 2
            for c in range(half):
                lanes = slice(c * LANES, (c + 1) * LANES)
                g_lanes = slice((half + c) * LANES, (half + c + 1) * LANES)
                xg_v[slot, :, lanes] = buf_x[pl.ds(c, chunk, stride=SUB), :].astype(jnp.bfloat16)
                xg_v[slot, :, g_lanes] = buf_g[pl.ds(half + c, chunk, stride=SUB), :].astype(jnp.bfloat16)
                if with_dy:
                    dy_v[slot, :, lanes] = buf_x[pl.ds(half + c, chunk, stride=SUB), :].astype(jnp.bfloat16)
            for copy in copies(e, j, slot):
                copy.start()
            return done + 1

        return lax.fori_loop(0, nt_ref[e * 2 + region], one_chunk, done)

    lax.fori_loop(0, exp_local, one_expert, 0)
    for slot in range(2):
        for copy in copies(0, 0, slot):
            copy.wait()


def gather_rows(tokens, slot_tok, slot_gate, nt, region, capacity, carried=()):
    with_dy = region == 0
    n_src = len(tokens)
    exp_local = nt.shape[0]
    chunk = capacity // CHUNKS
    tok_dev = tokens[0].shape[0]
    width = SUB * LANES
    tile_rows = n_src * chunk
    hbm = pl.BlockSpec(memory_space=pl.ANY)
    per_src = pl.BlockSpec((1, 1, slot_tok.shape[2]), lambda s, *_: (s, 0, 0), memory_space=pltpu.SMEM)
    out_shape = [jax.ShapeDtypeStruct((exp_local, 2, CHUNKS, tile_rows, width), jnp.bfloat16)]
    if with_dy:
        out_shape.append(jax.ShapeDtypeStruct((exp_local, CHUNKS, tile_rows, width // 2), jnp.bfloat16))
    return pl.pallas_call(
        functools.partial(gather_kernel, n_src, with_dy, region, exp_local, capacity, chunk),
        grid_spec=pltpu.PrefetchScalarGridSpec(
            num_scalar_prefetch=1,
            grid=(n_src,),
            in_specs=[per_src, per_src] + [hbm] * (n_src + len(carried)),
            out_specs=[hbm] * len(out_shape),
            scratch_shapes=[
                pltpu.VMEM((tok_dev, SUB, LANES), jnp.bfloat16),
                pltpu.VMEM((chunk * SUB, LANES), jnp.float32),
                pltpu.VMEM((chunk * SUB, LANES), jnp.float32),
                pltpu.VMEM((2, chunk, width), jnp.bfloat16),
                pltpu.VMEM((2, chunk, width // 2), jnp.bfloat16),
                pltpu.SemaphoreType.DMA((2,)),
                pltpu.SemaphoreType.DMA((2,)),
                pltpu.SemaphoreType.DMA,
            ]),
        out_shape=out_shape,
        input_output_aliases={3 + n_src + k: k for k in range(len(carried))},
        compiler_params=pltpu.CompilerParams(dimension_semantics=("arbitrary",), vmem_limit_bytes=VMEM_BYTES),
        interpret=INTERPRET,
    )(nt.reshape(-1), slot_tok, slot_gate, *tokens, *carried)


def dot(a, b, dims):
    return lax.dot_general(a, b, (dims, ((), ())), preferred_element_type=jnp.float32)


NN, NT, TN = ((1,), (0,)), ((1,), (1,)), ((0,), (0,))


def expert_kernel(e0, step_rows, nt_ref, mine_ref, xg_ref, dy_ref, w1o, w1p, w3o, w3p, w2o, w2p, *refs):
    *dx_refs, dr_ref = refs[len(refs) - 10 - 1 - N_OWN:-10]
    dw1_ref, dw3_ref, dw2_ref, h1, h3, da, hid, dh1, dh3, dw2t = refs[-10:]
    e = pl.program_id(0)
    t = pl.program_id(1)
    region, j = t // CHUNKS, t % CHUNKS
    half = w1o.shape[1]
    d_model = 2 * half
    mine = pl.multiple_of(mine_ref[0] * half, half)
    other = pl.multiple_of(half - mine_ref[0] * half, half)

    @pl.when(t == 0)
    def _():
        dw1_ref[...] = jnp.zeros_like(dw1_ref)
        dw3_ref[...] = jnp.zeros_like(dw3_ref)
        dw2t[...] = jnp.zeros_like(dw2t)

    @pl.when(j < nt_ref[(e0 + e) * 2 + region])
    def _():
        xo = xg_ref[0, 0, 0, :, pl.ds(mine, half)]
        xp = xg_ref[0, 0, 0, :, pl.ds(other, half)]
        go = xg_ref[0, 0, 0, :, pl.ds(d_model + mine, half)]
        gp = xg_ref[0, 0, 0, :, pl.ds(d_model + other, half)]
        h1[...] = dot(xo, w1o[0], NN) + dot(xp, w1p[0], NN)
        h3[...] = dot(xo, w3o[0], NN) + dot(xp, w3p[0], NN)
        da[...] = dot(go, w2o[0], NT) + dot(gp, w2p[0], NT)

        def rows(k, carry):
            at = pl.ds(pl.multiple_of(k * step_rows, step_rows), step_rows)
            p1, p3, d = h1[at, :], h3[at, :], da[at, :]
            s = jax.nn.sigmoid(p1)
            hid[at, :] = (p1 * s * p3).astype(jnp.bfloat16)
            dh1[at, :] = (d * p3 * s * (1.0 + p1 * (1.0 - s))).astype(jnp.bfloat16)
            dh3[at, :] = (d * p1 * s).astype(jnp.bfloat16)
            return carry

        lax.fori_loop(0, h1.shape[0] // step_rows, rows, 0)
        dw1_ref[0] += dot(xo, dh1[...], TN)
        dw3_ref[0] += dot(xo, dh3[...], TN)
        dw2t[...] += dot(go, hid[...], TN)

    @pl.when((region == 0) & (j < nt_ref[(e0 + e) * 2]))
    def _():
        dyo = dy_ref[0, 0, :, pl.ds(mine, half)].astype(jnp.float32)
        dyp = dy_ref[0, 0, :, pl.ds(other, half)].astype(jnp.float32)
        prod = dyo * dot(hid[...], w2o[0], NN) + dyp * dot(hid[...], w2p[0], NN)
        dr = jnp.sum(prod, axis=1, keepdims=True)
        dr_ref[0, 0] = jnp.broadcast_to(dr, (dr.shape[0], LANES)).T[:1]
        dxo = (dot(dh1[...], w1o[0], NT) + dot(dh3[...], w3o[0], NT)).astype(jnp.bfloat16)
        dxp = (dot(dh1[...], w1p[0], NT) + dot(dh3[...], w3p[0], NT)).astype(jnp.bfloat16)
        chunk = dx_refs[0].shape[2]
        for k, dx_ref in enumerate(dx_refs):
            dx_ref[0, 0, :, pl.ds(mine, half)] = dxo[k * chunk:(k + 1) * chunk]
            dx_ref[0, 0, :, pl.ds(other, half)] = dxp[k * chunk:(k + 1) * chunk]

    @pl.when(t == pl.num_programs(1) - 1)
    def _():
        dw2_ref[0] = dw2t[...].T


def expert_group(e0, count, xg, dy, nt, mine, own, peer, carried):
    exp_local, _, _, tile_rows, width = xg.shape
    half, d_ff = own[0].shape[1:]
    step_rows = 16
    chunk = tile_rows // N_OWN

    def own_tile(e, t, nt_ref, _):
        return (e0 + e, jnp.minimum(jnp.where(t < CHUNKS, t, CHUNKS - 1), nt_ref[(e0 + e) * 2] - 1), 0, 0)

    def own_rows(e, t, nt_ref, _):
        return (e, jnp.minimum(jnp.where(t < CHUNKS, t, CHUNKS - 1), nt_ref[(e0 + e) * 2] - 1), 0, 0)

    def xg_tile(e, t, nt_ref, _):
        region = t // CHUNKS
        return (e0 + e, region, jnp.minimum(t % CHUNKS, nt_ref[(e0 + e) * 2 + region] - 1), 0, 0)

    at_own = lambda e, t, *_: (e0 + e, 0, 0)
    at_peer = lambda e, t, *_: (e, 0, 0)
    up = lambda at: pl.BlockSpec((1, half, d_ff), at)
    down = lambda at: pl.BlockSpec((1, d_ff, half), at)
    out_shape = [
        *[jax.ShapeDtypeStruct((count, CHUNKS, chunk, width // 2), jnp.bfloat16)] * N_OWN,
        jax.ShapeDtypeStruct((exp_local, CHUNKS, 1, tile_rows), jnp.float32),
        jax.ShapeDtypeStruct((exp_local, half, d_ff), jnp.float32),
        jax.ShapeDtypeStruct((exp_local, half, d_ff), jnp.float32),
        jax.ShapeDtypeStruct((exp_local, d_ff, half), jnp.float32),
    ]
    n_in = 2 + 8
    carried = list(carried)
    return pl.pallas_call(
        functools.partial(expert_kernel, e0, step_rows),
        grid_spec=pltpu.PrefetchScalarGridSpec(
            num_scalar_prefetch=2,
            grid=(count, 2 * CHUNKS),
            in_specs=[
                pl.BlockSpec((1, 1, 1, tile_rows, width), xg_tile),
                pl.BlockSpec((1, 1, tile_rows, width // 2), own_tile),
                up(at_own), up(at_peer), up(at_own), up(at_peer), down(at_own), down(at_peer),
            ] + [pl.BlockSpec(memory_space=pl.ANY)] * len(carried),
            out_specs=[
                *[pl.BlockSpec((1, 1, chunk, width // 2), own_rows)] * N_OWN,
                pl.BlockSpec((1, 1, 1, tile_rows), own_tile),
                up(at_own), up(at_own), down(at_own),
            ],
            scratch_shapes=[
                pltpu.VMEM((tile_rows, d_ff), jnp.float32),
                pltpu.VMEM((tile_rows, d_ff), jnp.float32),
                pltpu.VMEM((tile_rows, d_ff), jnp.float32),
                pltpu.VMEM((tile_rows, d_ff), jnp.bfloat16),
                pltpu.VMEM((tile_rows, d_ff), jnp.bfloat16),
                pltpu.VMEM((tile_rows, d_ff), jnp.bfloat16),
                pltpu.VMEM((half, d_ff), jnp.float32),
            ]),
        out_shape=out_shape,
        input_output_aliases={n_in + k: N_OWN + k for k in range(len(carried))},
        compiler_params=pltpu.CompilerParams(
            dimension_semantics=("arbitrary", "arbitrary"), vmem_limit_bytes=VMEM_BYTES),
        interpret=INTERPRET,
    )(nt.reshape(-1), mine, xg, dy, own[0], peer[0], own[1], peer[1], own[2], peer[2], *carried)


def combine_kernel(stage, counts, e0, exp_local, capacity, chunk, tok_ref, dr_ref, *refs):
    stride = capacity + PAD
    n_exp = sum(counts)
    rows_hbm = refs[:N_OWN * len(counts)]
    refs = refs[N_OWN * len(counts):]
    first, last = stage == 0, stage == len(STAGES) - 1
    if not first:
        acc_in, refs = refs[0], refs[1:]
    if last:
        gx_out, dr_out, acc, tmp, rows_v, sem, acc_sem = refs
    else:
        acc_out, acc, tmp, rows_v, sem, acc_sem = refs
    src = pl.program_id(0)
    tok_dev = acc.shape[0] // SUB - 1

    def count_of(k, e):
        return tok_ref[(k * exp_local + e0 + e) * stride + capacity + 1]

    def tiles(n):
        return (n + chunk - 1) // chunk

    def start(k):
        base = 0
        for g, count in enumerate(counts):
            ref = rows_hbm[g * N_OWN + k]

            def per_expert(e, carry, ref=ref, base=base):
                def one(j, c):
                    at = (base + e) * CHUNKS + j
                    pltpu.make_async_copy(ref.at[e, j], rows_v.at[k % 2, at], sem.at[k % 2, at]).start()
                    return c

                return lax.fori_loop(0, tiles(count_of(k, base + e)), one, carry)

            lax.fori_loop(0, count, per_expert, 0)
            base += count

    @pl.when(src == 0)
    def _():
        if not first:
            load = pltpu.make_async_copy(acc_in, acc, acc_sem)
            load.start()
        start(0)
        tmp[...] = jnp.zeros_like(tmp)
        if first:
            acc[...] = jnp.zeros_like(acc)
        else:
            load.wait()

    for k in range(1, N_OWN):
        @pl.when(src == k - 1)
        def _(k=k):
            start(k)

    buf = lax.rem(src, 2)
    sub = lax.broadcasted_iota(jnp.int32, (SUB, LANES), 0)
    lane = lax.broadcasted_iota(jnp.int32, (SUB, LANES), 1)

    def per_expert(e, carry):
        n = count_of(src, e)
        here = (sub == SUB // 2) & (lane == src * exp_local + e0 + e)

        def one(j, c):
            at = e * CHUNKS + j
            pltpu.make_async_copy(rows_hbm[0].at[0, 0], rows_v.at[buf, at], sem.at[buf, at]).wait()
            for c4 in range(SUB // 2):
                tmp[pl.ds(c4, chunk, stride=SUB), :] = rows_v[
                    buf, at, :, c4 * LANES:(c4 + 1) * LANES].astype(jnp.float32)
            slots = (src * exp_local + e0 + e) * stride + j * chunk
            drs = (src * n_exp + e) * capacity + j * chunk

            def rows(r8, c):
                r0 = r8 * 8
                toks = [jnp.where(j * chunk + r0 + u < n, tok_ref[slots + r0 + u], tok_dev) for u in range(8)]
                ats = [pl.ds(pl.multiple_of(t * SUB, SUB), SUB) for t in toks]
                sums = [acc[ats[u], :] + jnp.where(
                    here, dr_ref[drs + r0 + u], tmp[pl.ds(pl.multiple_of((r0 + u) * SUB, SUB), SUB), :])
                    for u in range(8)]
                for u in range(8):
                    acc[ats[u], :] = sums[u]
                return c

            lax.fori_loop(0, (jnp.minimum(n - j * chunk, chunk) + 7) // 8, rows, 0)
            return c

        return lax.fori_loop(0, tiles(n), one, carry)

    lax.fori_loop(0, n_exp, per_expert, 0)

    @pl.when(src == N_OWN - 1)
    def _():
        if last:
            for c in range(SUB // 2):
                gx_out[:, c * LANES:(c + 1) * LANES] = acc[pl.ds(c, tok_dev, stride=SUB), :].astype(jnp.bfloat16)
            dr_out[...] = acc[pl.ds(SUB // 2, tok_dev, stride=SUB), :]
        else:
            store = pltpu.make_async_copy(acc, acc_out, acc_sem)
            store.start()
            store.wait()


def combine(stage, slot_home, dr, rows, carried, exp_local, capacity, tok_dev):
    counts = [GROUPS[g] for g in STAGES[stage]]
    e0 = sum(GROUPS[:STAGES[stage][0]])
    n_exp = sum(counts)
    chunk, d_model = rows[0].shape[2:]
    smem = pl.BlockSpec(memory_space=pltpu.SMEM)
    hbm = pl.BlockSpec(memory_space=pl.ANY)
    acc_shape = ((tok_dev + 1) * SUB, LANES)
    if stage == len(STAGES) - 1:
        out_specs = [pl.BlockSpec((tok_dev, d_model), lambda s: (0, 0)), pl.BlockSpec((tok_dev, LANES), lambda s: (0, 0))]
        out_shape = [jax.ShapeDtypeStruct((tok_dev, d_model), jnp.bfloat16),
                     jax.ShapeDtypeStruct((tok_dev, LANES), jnp.float32)]
    else:
        out_specs = [hbm]
        out_shape = [jax.ShapeDtypeStruct(acc_shape, jnp.float32)]
    return pl.pallas_call(
        functools.partial(combine_kernel, stage, counts, e0, exp_local, capacity, chunk),
        grid=(N_OWN,),
        in_specs=[smem, smem] + [hbm] * (len(rows) + len(carried)),
        out_specs=out_specs,
        out_shape=out_shape,
        scratch_shapes=[
            pltpu.VMEM(acc_shape, jnp.float32),
            pltpu.VMEM((chunk * SUB, LANES), jnp.float32),
            pltpu.VMEM((2, n_exp * CHUNKS, chunk, d_model), jnp.bfloat16),
            pltpu.SemaphoreType.DMA((2, n_exp * CHUNKS)),
            pltpu.SemaphoreType.DMA,
        ],
        compiler_params=pltpu.CompilerParams(
            dimension_semantics=("arbitrary",), vmem_limit_bytes=VMEM_BYTES),
        interpret=INTERPRET,
    )(slot_home, dr, *rows, *carried)


def solution(mesh):
    n_ep = mesh.shape["ep"]
    n_fsdp = mesh.shape["fsdp"]
    tok_spec = P(("fsdp", "ep"), None)
    spec_in = P("ep", "fsdp", None)
    spec_out = P("ep", None, "fsdp")

    def swap(value, axis, mask):
        size = n_fsdp if axis == "fsdp" else n_ep
        return lax.ppermute(value, axis, [(k, k ^ mask) for k in range(size)])

    def per_device(x_tok, dy_tok, expert_ids, route_w, w_gate, w_up, w_down):
        tok_dev, top_k = expert_ids.shape
        exp_local = w_gate.shape[0]
        experts = exp_local * n_ep
        capacity = capacity_of(tok_dev, top_k, experts)
        chunk = capacity // CHUNKS
        my_fsdp = lax.axis_index("fsdp")
        my_ep = lax.axis_index("ep")

        tokens = jnp.concatenate([x_tok, dy_tok], axis=1).reshape(tok_dev, SUB, LANES)
        tok_y = swap(tokens, "fsdp", 1)
        tok_x = swap(tokens, "ep", 2)
        tok_c = swap(tokens, "ep", 1)
        tok_yx = swap(tok_y, "ep", 2)
        tok_cx = swap(tok_x, "ep", 1)
        tok_cy = swap(tok_y, "ep", 1)
        tok_cyx = swap(tok_yx, "ep", 1)
        all_tokens = (tokens, tok_c, tok_x, tok_cx, tok_y, tok_cy, tok_yx, tok_cyx)

        slot_tok, slot_gate = route_slots(
            expert_ids.reshape(-1), route_w.reshape(-1), top_k, experts, capacity)
        slot_home = slot_tok.reshape(n_ep, -1)
        slot_home = jnp.stack(
            [lax.dynamic_index_in_dim(slot_home, my_ep ^ b, axis=0, keepdims=False) for b in range(n_ep)]).reshape(-1)
        slot_tok = lax.all_gather(slot_tok, ("fsdp", "ep"), axis=0, tiled=False)
        slot_gate = lax.all_gather(slot_gate, ("fsdp", "ep"), axis=0, tiled=False)

        def for_me(v):
            v = v.reshape(n_fsdp * n_ep, n_ep, -1)
            v = lax.dynamic_index_in_dim(v, my_ep, axis=1, keepdims=False)
            order = [(my_fsdp ^ a) * n_ep + (my_ep ^ b) for a in range(n_fsdp) for b in range(n_ep)]
            return jnp.stack([lax.dynamic_index_in_dim(v, k, axis=0, keepdims=True) for k in order])

        slot_tok, slot_gate = for_me(slot_tok), for_me(slot_gate)
        cnt = slot_tok.reshape(n_fsdp, n_ep, exp_local, capacity + PAD)[..., capacity + 1]
        most = jnp.max(cnt, axis=1)
        nt = jnp.maximum((most + chunk - 1) // chunk, 1).T

        xg, dy = gather_rows(all_tokens[:n_ep], slot_tok[:n_ep], slot_gate[:n_ep], nt, 0, capacity)
        xg, = gather_rows(all_tokens[n_ep:], slot_tok[n_ep:], slot_gate[n_ep:], nt, 1, capacity, (xg,))

        own = (w_gate, w_up, w_down)
        mine = my_fsdp.astype(jnp.int32).reshape(1)
        carried, sums = (), ()
        e0 = 0
        rows = []
        for g, count in enumerate(GROUPS):
            peer = [swap(w[e0:e0 + count], "fsdp", 1) for w in own]
            out = expert_group(e0, count, xg, dy, nt, mine, own, peer, carried)
            dx_g, carried = out[:n_ep], out[n_ep:]
            rows += [dx_g[0]] + [swap(dx_g[b], "ep", b) for b in range(1, n_ep)]
            e0 += count
            for stage, groups in enumerate(STAGES):
                if g == groups[-1]:
                    dr = carried[0][e0 - sum(GROUPS[k] for k in groups):e0].reshape(-1, CHUNKS, n_ep, chunk)
                    dr = dr.transpose(2, 0, 1, 3).reshape(n_ep, -1)
                    dr = jnp.concatenate(
                        [dr[0]] + [swap(dr[b], "ep", b) for b in range(1, n_ep)])
                    sums = combine(stage, slot_home, dr, rows, sums, exp_local, capacity, tok_dev)
                    rows = []
        _, grad_w_gate, grad_w_up, grad_w_down = carried
        grad_x, dr_tok = sums
        place = ((expert_ids // exp_local) ^ my_ep) * exp_local + expert_ids % exp_local
        hit = place[:, :, None] == jnp.arange(LANES, dtype=jnp.int32)
        route_grad = jnp.sum(jnp.where(hit, dr_tok[:, None, :], 0.0), axis=2)
        return grad_x, route_grad, grad_w_gate, grad_w_up, grad_w_down

    return jax.shard_map(
        per_device, mesh=mesh,
        in_specs=(tok_spec, tok_spec, tok_spec, tok_spec, spec_in, spec_in, spec_out),
        out_specs=(tok_spec, tok_spec, spec_in, spec_in, spec_out),
        check_vma=False)
```

```python
import functools

import jax
import jax.numpy as jnp
from jax import lax
from jax.experimental import pallas as pl
from jax.experimental.pallas import tpu as pltpu
from jax.sharding import PartitionSpec as P


CAP_FACTOR = 3
CHUNKS = 4
GROUPS = (4, 4, 2, 2, 2, 1, 1)
STAGES = ((0, 1, 2), (3, 4, 5, 6))
PAD = 8
LANES = 128
N_OWN = 4
SUB = 8
INTERPRET = False
VMEM_BYTES = 67_043_328


def capacity_of(tok_dev, top_k, experts):
    return max(8, ((CAP_FACTOR * tok_dev * top_k // experts + 7) // 8) * 8)


def route_kernel(n_pairs, top_k, experts, capacity, ids_ref, gate_ref, tok_ref, slot_gate_ref, cnt_ref):
    stride = capacity + PAD
    for e in range(experts):
        cnt_ref[e] = 0

    def step(t, carry):
        ids = [ids_ref[t * top_k + j] for j in range(top_k)]
        gates = [gate_ref[t * top_k + j] for j in range(top_k)]
        counts = [cnt_ref[e] for e in ids]
        for j in range(top_k):
            slot = ids[j] * stride + jnp.minimum(counts[j], capacity)
            tok_ref[slot] = t
            slot_gate_ref[slot] = gates[j]
            cnt_ref[ids[j]] = counts[j] + 1
        return carry

    lax.fori_loop(0, n_pairs // top_k, step, 0, unroll=2)
    for e in range(experts):
        tok_ref[e * stride + capacity + 1] = jnp.minimum(cnt_ref[e], capacity)


def route_slots(ids_flat, gates_flat, top_k, experts, capacity):
    n_pairs = ids_flat.shape[0]
    smem = pl.BlockSpec(memory_space=pltpu.SMEM)
    words = experts * (capacity + PAD)
    return pl.pallas_call(
        functools.partial(route_kernel, n_pairs, top_k, experts, capacity),
        in_specs=[smem, smem],
        out_specs=[smem, smem],
        out_shape=[jax.ShapeDtypeStruct((words,), jnp.int32), jax.ShapeDtypeStruct((words,), jnp.float32)],
        scratch_shapes=[pltpu.SMEM((experts,), jnp.int32)],
        name="route",
        interpret=INTERPRET,
    )(ids_flat, gates_flat)


def gather_kernel(n_src, with_dy, region, exp_local, capacity, chunk, nt_ref, tok_ref, gate_ref, *refs):
    stride = capacity + PAD
    token_refs = refs[:n_src]
    refs = list(refs[n_src if with_dy else n_src + 1:])
    xg_hbm = refs.pop(0)
    dy_hbm = refs.pop(0) if with_dy else None
    rows_v, buf_x, buf_g, xg_v, dy_v, xg_sem, dy_sem, tok_sem = refs
    src = pl.program_id(0)
    for k in range(n_src):
        @pl.when(src == k)
        def _(k=k):
            copy = pltpu.make_async_copy(token_refs[k], rows_v, tok_sem)
            copy.start()
            copy.wait()

    def copies(e, j, slot):
        at = pl.ds(src * chunk, chunk)
        out = [pltpu.make_async_copy(xg_v.at[slot], xg_hbm.at[e, region, j, at], xg_sem.at[slot])]
        if with_dy:
            out.append(pltpu.make_async_copy(dy_v.at[slot], dy_hbm.at[e, j, at], dy_sem.at[slot]))
        return out

    is_x = lax.broadcasted_iota(jnp.int32, (SUB, LANES), 0) < SUB // 2
    from_g = buf_g if with_dy else buf_x

    def one_expert(e, done):
        def one_chunk(j, done):
            slot = lax.rem(done, 2)

            @pl.when(done >= 2)
            def _():
                for copy in copies(e, j, slot):
                    copy.wait()

            def rows(r8, carry):
                at0 = e * stride + j * chunk + r8 * 8
                toks = [tok_ref[0, 0, at0 + u] for u in range(8)]
                gates = [gate_ref[0, 0, at0 + u] for u in range(8)]
                loaded = [rows_v[t].astype(jnp.float32) for t in toks]
                for u in range(8):
                    at = pl.ds(pl.multiple_of((r8 * 8 + u) * SUB, SUB), SUB)
                    if with_dy:
                        buf_x[at, :] = loaded[u]
                        buf_g[at, :] = loaded[u] * gates[u]
                    else:
                        buf_x[at, :] = loaded[u] * jnp.where(is_x, 1.0, gates[u])
                return carry

            lax.fori_loop(0, chunk // 8, rows, 0)
            half = SUB // 2
            for c in range(half):
                lanes = slice(c * LANES, (c + 1) * LANES)
                g_lanes = slice((half + c) * LANES, (half + c + 1) * LANES)
                xg_v[slot, :, lanes] = buf_x[pl.ds(c, chunk, stride=SUB), :].astype(jnp.bfloat16)
                xg_v[slot, :, g_lanes] = from_g[pl.ds(half + c, chunk, stride=SUB), :].astype(jnp.bfloat16)
                if with_dy:
                    dy_v[slot, :, lanes] = buf_x[pl.ds(half + c, chunk, stride=SUB), :].astype(jnp.bfloat16)
            for copy in copies(e, j, slot):
                copy.start()
            return done + 1

        return lax.fori_loop(0, nt_ref[e * 2 + region], one_chunk, done)

    lax.fori_loop(0, exp_local, one_expert, 0)
    for slot in range(2):
        for copy in copies(0, 0, slot):
            copy.wait()


def gather_rows(tokens, slot_tok, slot_gate, nt, region, capacity, carried=()):
    with_dy = region == 0
    n_src = len(tokens)
    exp_local = nt.shape[0]
    chunk = capacity // CHUNKS
    tok_dev = tokens[0].shape[0]
    width = SUB * LANES
    tile_rows = n_src * chunk
    hbm = pl.BlockSpec(memory_space=pl.ANY)
    per_src = pl.BlockSpec((1, 1, slot_tok.shape[2]), lambda s, *_: (s, 0, 0), memory_space=pltpu.SMEM)
    out_shape = [jax.ShapeDtypeStruct((exp_local, 2, CHUNKS, tile_rows, width), jnp.bfloat16)]
    if with_dy:
        out_shape.append(jax.ShapeDtypeStruct((exp_local, CHUNKS, tile_rows, width // 2), jnp.bfloat16))
    return pl.pallas_call(
        functools.partial(gather_kernel, n_src, with_dy, region, exp_local, capacity, chunk),
        grid_spec=pltpu.PrefetchScalarGridSpec(
            num_scalar_prefetch=1,
            grid=(n_src,),
            in_specs=[per_src, per_src] + [hbm] * (n_src + len(carried)),
            out_specs=[hbm] * len(out_shape),
            scratch_shapes=[
                pltpu.VMEM((tok_dev, SUB, LANES), jnp.bfloat16),
                pltpu.VMEM((chunk * SUB, LANES), jnp.float32),
                pltpu.VMEM((chunk * SUB, LANES), jnp.float32),
                pltpu.VMEM((2, chunk, width), jnp.bfloat16),
                pltpu.VMEM((2, chunk, width // 2), jnp.bfloat16),
                pltpu.SemaphoreType.DMA((2,)),
                pltpu.SemaphoreType.DMA((2,)),
                pltpu.SemaphoreType.DMA,
            ]),
        out_shape=out_shape,
        input_output_aliases={3 + n_src + k: k for k in range(len(carried))},
        compiler_params=pltpu.CompilerParams(dimension_semantics=("arbitrary",), vmem_limit_bytes=VMEM_BYTES),
        interpret=INTERPRET,
    )(nt.reshape(-1), slot_tok, slot_gate, *tokens, *carried)


def dot(a, b, dims):
    return lax.dot_general(a, b, (dims, ((), ())), preferred_element_type=jnp.float32)


NN, NT, TN = ((1,), (0,)), ((1,), (1,)), ((0,), (0,))


def expert_kernel(step_rows, nt_ref, steps_ref, meta_ref, xg_ref, dy_ref, w1o, w1p, w3o, w3p, w2o, w2p, *refs):
    *dx_refs, dr_ref = refs[len(refs) - 10 - 1 - N_OWN:-10]
    dw1_ref, dw3_ref, dw2_ref, h1, h3, da, hid, dh1, dh3, dw2t = refs[-10:]
    step = pl.program_id(0)
    code = steps_ref[meta_ref[1] + step]
    e, j = code // CHUNKS, code % CHUNKS
    half = w1o.shape[1]
    d_model = 2 * half
    mine = pl.multiple_of(meta_ref[0] * half, half)
    other = pl.multiple_of(half - meta_ref[0] * half, half)

    @pl.when((step < meta_ref[2]) & (j == 0))
    def _():
        dw1_ref[...] = jnp.zeros_like(dw1_ref)
        dw3_ref[...] = jnp.zeros_like(dw3_ref)
        dw2t[...] = jnp.zeros_like(dw2t)

    def tile(region):
        xo = xg_ref[0, region, 0, :, pl.ds(mine, half)]
        xp = xg_ref[0, region, 0, :, pl.ds(other, half)]
        go = xg_ref[0, region, 0, :, pl.ds(d_model + mine, half)]
        gp = xg_ref[0, region, 0, :, pl.ds(d_model + other, half)]
        h1[...] = dot(xo, w1o[0], NN) + dot(xp, w1p[0], NN)
        h3[...] = dot(xo, w3o[0], NN) + dot(xp, w3p[0], NN)
        da[...] = dot(go, w2o[0], NT) + dot(gp, w2p[0], NT)

        def rows(k, carry):
            at = pl.ds(pl.multiple_of(k * step_rows, step_rows), step_rows)
            p1, p3, d = h1[at, :], h3[at, :], da[at, :]
            s = jax.nn.sigmoid(p1)
            hid[at, :] = (p1 * s * p3).astype(jnp.bfloat16)
            dh1[at, :] = (d * p3 * s * (1.0 + p1 * (1.0 - s))).astype(jnp.bfloat16)
            dh3[at, :] = (d * p1 * s).astype(jnp.bfloat16)
            return carry

        lax.fori_loop(0, h1.shape[0] // step_rows, rows, 0)
        dw1_ref[0] += dot(xo, dh1[...], TN)
        dw3_ref[0] += dot(xo, dh3[...], TN)
        dw2t[...] += dot(go, hid[...], TN)

        @pl.when(region == 0)
        def _():
            dyo = dy_ref[0, 0, :, pl.ds(mine, half)].astype(jnp.float32)
            dyp = dy_ref[0, 0, :, pl.ds(other, half)].astype(jnp.float32)
            prod = dyo * dot(hid[...], w2o[0], NN) + dyp * dot(hid[...], w2p[0], NN)
            dr = jnp.sum(prod, axis=1, keepdims=True)
            dr_ref[0, 0] = jnp.broadcast_to(dr, (dr.shape[0], LANES)).T[:1]
            dxo = (dot(dh1[...], w1o[0], NT) + dot(dh3[...], w3o[0], NT)).astype(jnp.bfloat16)
            dxp = (dot(dh1[...], w1p[0], NT) + dot(dh3[...], w3p[0], NT)).astype(jnp.bfloat16)
            chunk = dx_refs[0].shape[2]
            for k, dx_ref in enumerate(dx_refs):
                dx_ref[0, 0, :, pl.ds(mine, half)] = dxo[k * chunk:(k + 1) * chunk]
                dx_ref[0, 0, :, pl.ds(other, half)] = dxp[k * chunk:(k + 1) * chunk]

    def one_region(region, carry):
        @pl.when((step < meta_ref[2]) & (j < nt_ref[e * 2 + region]))
        def _():
            tile(region)

        return carry

    lax.fori_loop(0, 2, one_region, 0)

    @pl.when((step < meta_ref[2]) & (j == jnp.maximum(nt_ref[e * 2], nt_ref[e * 2 + 1]) - 1))
    def _():
        dw2_ref[0] = dw2t[...].T


def expert_group(e0, count, xg, dy, nt, steps, meta, own, peer, carried):
    exp_local, _, _, tile_rows, width = xg.shape
    half, d_ff = own[0].shape[1:]
    step_rows = 16
    chunk = tile_rows // N_OWN

    def place(s, steps_ref, meta_ref):
        code = steps_ref[meta_ref[1] + jnp.minimum(s, meta_ref[2] - 1)]
        return code // CHUNKS, code % CHUNKS

    def own_tile(s, nt_ref, steps_ref, meta_ref):
        e, j = place(s, steps_ref, meta_ref)
        return (e, jnp.minimum(j, nt_ref[e * 2] - 1), 0, 0)

    def own_rows(s, nt_ref, steps_ref, meta_ref):
        e, j = place(s, steps_ref, meta_ref)
        return (e - e0, jnp.minimum(j, nt_ref[e * 2] - 1), 0, 0)

    def xg_tile(s, nt_ref, steps_ref, meta_ref):
        e, j = place(s, steps_ref, meta_ref)
        return (e, 0, j, 0, 0)

    def at_own(s, nt_ref, steps_ref, meta_ref):
        return (place(s, steps_ref, meta_ref)[0], 0, 0)

    def at_peer(s, nt_ref, steps_ref, meta_ref):
        return (place(s, steps_ref, meta_ref)[0] - e0, 0, 0)

    up = lambda at: pl.BlockSpec((1, half, d_ff), at)
    down = lambda at: pl.BlockSpec((1, d_ff, half), at)
    out_shape = [
        *[jax.ShapeDtypeStruct((count, CHUNKS, chunk, width // 2), jnp.bfloat16)] * N_OWN,
        jax.ShapeDtypeStruct((exp_local, CHUNKS, 1, tile_rows), jnp.float32),
        jax.ShapeDtypeStruct((exp_local, half, d_ff), jnp.float32),
        jax.ShapeDtypeStruct((exp_local, half, d_ff), jnp.float32),
        jax.ShapeDtypeStruct((exp_local, d_ff, half), jnp.float32),
    ]
    n_in = 3 + 8
    carried = list(carried)
    return pl.pallas_call(
        functools.partial(expert_kernel, step_rows),
        grid_spec=pltpu.PrefetchScalarGridSpec(
            num_scalar_prefetch=3,
            grid=(count * CHUNKS,),
            in_specs=[
                pl.BlockSpec((1, 2, 1, tile_rows, width), xg_tile),
                pl.BlockSpec((1, 1, tile_rows, width // 2), own_tile),
                up(at_own), up(at_peer), up(at_own), up(at_peer), down(at_own), down(at_peer),
            ] + [pl.BlockSpec(memory_space=pl.ANY)] * len(carried),
            out_specs=[
                *[pl.BlockSpec((1, 1, chunk, width // 2), own_rows)] * N_OWN,
                pl.BlockSpec((1, 1, 1, tile_rows), own_tile),
                up(at_own), up(at_own), down(at_own),
            ],
            scratch_shapes=[
                pltpu.VMEM((tile_rows, d_ff), jnp.float32),
                pltpu.VMEM((tile_rows, d_ff), jnp.float32),
                pltpu.VMEM((tile_rows, d_ff), jnp.float32),
                pltpu.VMEM((tile_rows, d_ff), jnp.bfloat16),
                pltpu.VMEM((tile_rows, d_ff), jnp.bfloat16),
                pltpu.VMEM((tile_rows, d_ff), jnp.bfloat16),
                pltpu.VMEM((half, d_ff), jnp.float32),
            ]),
        out_shape=out_shape,
        input_output_aliases={n_in + k: N_OWN + k for k in range(len(carried))},
        compiler_params=pltpu.CompilerParams(
            dimension_semantics=("arbitrary",), vmem_limit_bytes=VMEM_BYTES),
        interpret=INTERPRET,
    )(nt.reshape(-1), steps, meta, xg, dy, own[0], peer[0], own[1], peer[1], own[2], peer[2], *carried)


def combine_kernel(stage, counts, e0, exp_local, capacity, chunk, tok_ref, dr_ref, *refs):
    stride = capacity + PAD
    n_exp = sum(counts)
    rows_hbm = refs[:N_OWN * len(counts)]
    refs = refs[N_OWN * len(counts):]
    first, last = stage == 0, stage == len(STAGES) - 1
    if not first:
        acc_in, refs = refs[0], refs[1:]
    if last:
        place_ref, gx_out, rg_out, acc, tmp, rows_v, sem, acc_sem = refs
    else:
        acc_out, acc, tmp, rows_v, sem, acc_sem = refs
    src = pl.program_id(0)
    tok_dev = acc.shape[0] // SUB - 1

    def count_of(k, e):
        return tok_ref[(k * exp_local + e0 + e) * stride + capacity + 1]

    def tiles(n):
        return (n + chunk - 1) // chunk

    def start(k):
        base = 0
        for g, count in enumerate(counts):
            ref = rows_hbm[g * N_OWN + k]

            def per_expert(e, carry, ref=ref, base=base):
                def one(j, c):
                    at = (base + e) * CHUNKS + j
                    pltpu.make_async_copy(ref.at[e, j], rows_v.at[k % 2, at], sem.at[k % 2, at]).start()
                    return c

                return lax.fori_loop(0, tiles(count_of(k, base + e)), one, carry)

            lax.fori_loop(0, count, per_expert, 0)
            base += count

    @pl.when(src == 0)
    def _():
        if not first:
            load = pltpu.make_async_copy(acc_in, acc, acc_sem)
            load.start()
        start(0)
        tmp[...] = jnp.zeros_like(tmp)
        if first:
            acc[...] = jnp.zeros_like(acc)
        else:
            load.wait()

    for k in range(1, N_OWN):
        @pl.when(src == k - 1)
        def _(k=k):
            start(k)

    buf = lax.rem(src, 2)
    sub = lax.broadcasted_iota(jnp.int32, (SUB, LANES), 0)
    lane = lax.broadcasted_iota(jnp.int32, (SUB, LANES), 1)

    def per_expert(e, carry):
        n = count_of(src, e)
        here = (sub == SUB // 2) & (lane == src * exp_local + e0 + e)

        def one(j, c):
            at = e * CHUNKS + j
            pltpu.make_async_copy(rows_hbm[0].at[0, 0], rows_v.at[buf, at], sem.at[buf, at]).wait()
            for c4 in range(SUB // 2):
                tmp[pl.ds(c4, chunk, stride=SUB), :] = rows_v[
                    buf, at, :, c4 * LANES:(c4 + 1) * LANES].astype(jnp.float32)
            slots = (src * exp_local + e0 + e) * stride + j * chunk
            drs = (src * n_exp + e) * capacity + j * chunk

            def rows(r8, c):
                r0 = r8 * 8
                toks = [tok_ref[slots + r0 + u] for u in range(8)]
                ats = [pl.ds(pl.multiple_of(t * SUB, SUB), SUB) for t in toks]
                sums = [acc[ats[u], :] + jnp.where(
                    here, dr_ref[drs + r0 + u], tmp[pl.ds(pl.multiple_of((r0 + u) * SUB, SUB), SUB), :])
                    for u in range(8)]
                for u in range(8):
                    acc[ats[u], :] = sums[u]
                return c

            lax.fori_loop(0, (jnp.minimum(n - j * chunk, chunk) + 7) // 8, rows, 0)
            return c

        return lax.fori_loop(0, tiles(n), one, carry)

    lax.fori_loop(0, n_exp, per_expert, 0)

    @pl.when(src == N_OWN - 1)
    def _():
        if last:
            for c in range(SUB // 2):
                gx_out[:, c * LANES:(c + 1) * LANES] = acc[pl.ds(c, tok_dev, stride=SUB), :].astype(jnp.bfloat16)
            by_expert = acc[pl.ds(SUB // 2, tok_dev, stride=SUB), :].T[:N_OWN * exp_local]
            lane_of = lax.broadcasted_iota(jnp.int32, by_expert.shape, 0)
            for k in range(place_ref.shape[0]):
                mine = jnp.where(lane_of == place_ref[k:k + 1, :], by_expert, 0.0)
                rg_out[k:k + 1, :] = jnp.sum(mine, axis=0, keepdims=True)
        else:
            store = pltpu.make_async_copy(acc, acc_out, acc_sem)
            store.start()
            store.wait()


def combine(stage, slot_home, dr, rows, carried, place, exp_local, capacity, tok_dev):
    counts = [GROUPS[g] for g in STAGES[stage]]
    e0 = sum(GROUPS[:STAGES[stage][0]])
    n_exp = sum(counts)
    chunk, d_model = rows[0].shape[2:]
    smem = pl.BlockSpec(memory_space=pltpu.SMEM)
    hbm = pl.BlockSpec(memory_space=pl.ANY)
    acc_shape = ((tok_dev + 1) * SUB, LANES)
    if stage == len(STAGES) - 1:
        out_specs = [pl.BlockSpec((tok_dev, d_model), lambda s: (0, 0)), pl.BlockSpec(place.shape, lambda s: (0, 0))]
        out_shape = [jax.ShapeDtypeStruct((tok_dev, d_model), jnp.bfloat16),
                     jax.ShapeDtypeStruct(place.shape, jnp.float32)]
        extra, extra_specs = [place], [pl.BlockSpec(place.shape, lambda s: (0, 0))]
    else:
        extra, extra_specs = [], []
        out_specs = [hbm]
        out_shape = [jax.ShapeDtypeStruct(acc_shape, jnp.float32)]
    return pl.pallas_call(
        functools.partial(combine_kernel, stage, counts, e0, exp_local, capacity, chunk),
        grid=(N_OWN,),
        in_specs=[smem, smem] + [hbm] * (len(rows) + len(carried)) + extra_specs,
        out_specs=out_specs,
        out_shape=out_shape,
        scratch_shapes=[
            pltpu.VMEM(acc_shape, jnp.float32),
            pltpu.VMEM((chunk * SUB, LANES), jnp.float32),
            pltpu.VMEM((2, n_exp * CHUNKS, chunk, d_model), jnp.bfloat16),
            pltpu.SemaphoreType.DMA((2, n_exp * CHUNKS)),
            pltpu.SemaphoreType.DMA,
        ],
        compiler_params=pltpu.CompilerParams(
            dimension_semantics=("arbitrary",), vmem_limit_bytes=VMEM_BYTES),
        interpret=INTERPRET,
    )(slot_home, dr, *rows, *carried, *extra)


def solution(mesh):
    n_ep = mesh.shape["ep"]
    n_fsdp = mesh.shape["fsdp"]
    tok_spec = P(("fsdp", "ep"), None)
    spec_in = P("ep", "fsdp", None)
    spec_out = P("ep", None, "fsdp")

    def swap(value, axis, mask):
        size = n_fsdp if axis == "fsdp" else n_ep
        return lax.ppermute(value, axis, [(k, k ^ mask) for k in range(size)])

    def per_device(x_tok, dy_tok, expert_ids, route_w, w_gate, w_up, w_down):
        tok_dev, top_k = expert_ids.shape
        exp_local = w_gate.shape[0]
        experts = exp_local * n_ep
        capacity = capacity_of(tok_dev, top_k, experts)
        chunk = capacity // CHUNKS
        my_fsdp = lax.axis_index("fsdp")
        my_ep = lax.axis_index("ep")

        tokens = jnp.concatenate([x_tok, dy_tok], axis=1).reshape(tok_dev, SUB, LANES)
        tok_y = swap(tokens, "fsdp", 1)
        tok_x = swap(tokens, "ep", 2)
        tok_c = swap(tokens, "ep", 1)
        tok_yx = swap(tok_y, "ep", 2)
        tok_cx = swap(tok_x, "ep", 1)
        tok_cy = swap(tok_y, "ep", 1)
        tok_cyx = swap(tok_yx, "ep", 1)
        all_tokens = (tokens, tok_c, tok_x, tok_cx, tok_y, tok_cy, tok_yx, tok_cyx)

        slot_tok, slot_gate = route_slots(
            expert_ids.reshape(-1), route_w.reshape(-1), top_k, experts, capacity)
        slot_home = slot_tok.reshape(n_ep, -1)
        slot_home = jnp.stack(
            [lax.dynamic_index_in_dim(slot_home, my_ep ^ b, axis=0, keepdims=False) for b in range(n_ep)]).reshape(-1)
        slot_tok = lax.all_gather(slot_tok, ("fsdp", "ep"), axis=0, tiled=False)
        slot_gate = lax.all_gather(slot_gate, ("fsdp", "ep"), axis=0, tiled=False)

        def for_me(v):
            v = v.reshape(n_fsdp * n_ep, n_ep, -1)
            v = lax.dynamic_index_in_dim(v, my_ep, axis=1, keepdims=False)
            order = [(my_fsdp ^ a) * n_ep + (my_ep ^ b) for a in range(n_fsdp) for b in range(n_ep)]
            return jnp.stack([lax.dynamic_index_in_dim(v, k, axis=0, keepdims=True) for k in order])

        stride = capacity + PAD
        word = jnp.arange(stride, dtype=jnp.int32)

        def filled(tok, empty):
            tok = tok.reshape(-1, exp_local, stride)
            held = word < tok[..., capacity + 1:capacity + 2]
            return jnp.where(held | (word == capacity + 1), tok, empty), held

        slot_tok, held = filled(for_me(slot_tok), 0)
        slot_gate = jnp.where(held, for_me(slot_gate).reshape(held.shape), 0.0)
        slot_home = filled(slot_home, tok_dev)[0].reshape(-1)
        cnt = slot_tok[..., capacity + 1].reshape(n_fsdp, n_ep, exp_local)
        slot_tok = slot_tok.reshape(n_fsdp * n_ep, 1, -1)
        slot_gate = slot_gate.reshape(n_fsdp * n_ep, 1, -1)
        most = jnp.max(cnt, axis=1)
        nt = jnp.maximum((most + chunk - 1) // chunk, 1).T
        per_expert = jnp.max(nt, axis=1)
        active = (jnp.arange(CHUNKS, dtype=jnp.int32) < per_expert[:, None]).reshape(-1)
        code = jnp.arange(active.shape[0], dtype=jnp.int32)
        before = jnp.sum(jnp.where((code[None, :] < code[:, None]) & active[None, :], 1, 0), axis=1)
        steps = jnp.sum(jnp.where((before[None, :] == code[:, None]) & active[None, :], code[None, :], 0), axis=1)
        first = [sum(GROUPS[:g]) for g in range(len(GROUPS))]
        n_steps = [jnp.sum(per_expert[first[g]:first[g] + GROUPS[g]]) for g in range(len(GROUPS))]
        starts = [jnp.sum(per_expert[:first[g]]) for g in range(len(GROUPS))]

        xg, dy = gather_rows(all_tokens[:n_ep], slot_tok[:n_ep], slot_gate[:n_ep], nt, 0, capacity)
        xg, = gather_rows(all_tokens[n_ep:], slot_tok[n_ep:], slot_gate[n_ep:], nt, 1, capacity, (xg,))

        own = (w_gate, w_up, w_down)
        mine = my_fsdp.astype(jnp.int32)
        place = (((expert_ids // exp_local) ^ my_ep) * exp_local + expert_ids % exp_local).T
        carried, sums = (), ()
        e0 = 0
        rows = []
        for g, count in enumerate(GROUPS):
            peer = [swap(w[e0:e0 + count], "fsdp", 1) for w in own]
            meta = jnp.stack([mine, starts[g], n_steps[g]])
            out = expert_group(e0, count, xg, dy, nt, steps, meta, own, peer, carried)
            dx_g, carried = out[:n_ep], out[n_ep:]
            rows += [dx_g[0]] + [swap(dx_g[b], "ep", b) for b in range(1, n_ep)]
            e0 += count
            for stage, groups in enumerate(STAGES):
                if g == groups[-1]:
                    dr = carried[0][e0 - sum(GROUPS[k] for k in groups):e0].reshape(-1, CHUNKS, n_ep, chunk)
                    dr = dr.transpose(2, 0, 1, 3).reshape(n_ep, -1)
                    dr = jnp.concatenate(
                        [dr[0]] + [swap(dr[b], "ep", b) for b in range(1, n_ep)])
                    sums = combine(stage, slot_home, dr, rows, sums, place, exp_local, capacity, tok_dev)
                    rows = []
        _, grad_w_gate, grad_w_up, grad_w_down = carried
        grad_x, route_grad = sums[0], sums[1].T
        return grad_x, route_grad, grad_w_gate, grad_w_up, grad_w_down

    return jax.shard_map(
        per_device, mesh=mesh,
        in_specs=(tok_spec, tok_spec, tok_spec, tok_spec, spec_in, spec_in, spec_out),
        out_specs=(tok_spec, tok_spec, spec_in, spec_in, spec_out),
        check_vma=False)
```

```python
import functools

import jax
import jax.numpy as jnp
from jax import lax
from jax.experimental import pallas as pl
from jax.experimental.pallas import tpu as pltpu
from jax.sharding import PartitionSpec as P


CAP_FACTOR = 3
CHUNKS = 4
GROUPS = (4, 2, 2, 2, 2, 2, 1, 1)
STAGES = ((0, 1, 2, 3), (4, 5, 6, 7))
PAD = 8
LANES = 128
N_OWN = 4
SUB = 8
INTERPRET = False
VMEM_BYTES = 67_043_328


def capacity_of(tok_dev, top_k, experts):
    return max(8, ((CAP_FACTOR * tok_dev * top_k // experts + 7) // 8) * 8)


def route_kernel(n_pairs, top_k, experts, capacity, ids_ref, gate_ref, tok_ref, slot_gate_ref, cnt_ref):
    stride = capacity + PAD
    for e in range(experts):
        cnt_ref[e] = 0

    def step(t, carry):
        ids = [ids_ref[t * top_k + j] for j in range(top_k)]
        gates = [gate_ref[t * top_k + j] for j in range(top_k)]
        counts = [cnt_ref[e] for e in ids]
        for j in range(top_k):
            slot = ids[j] * stride + jnp.minimum(counts[j], capacity)
            tok_ref[slot] = t
            slot_gate_ref[slot] = gates[j]
            cnt_ref[ids[j]] = counts[j] + 1
        return carry

    lax.fori_loop(0, n_pairs // top_k, step, 0, unroll=2)
    for e in range(experts):
        tok_ref[e * stride + capacity + 1] = jnp.minimum(cnt_ref[e], capacity)


def route_slots(ids_flat, gates_flat, top_k, experts, capacity):
    n_pairs = ids_flat.shape[0]
    smem = pl.BlockSpec(memory_space=pltpu.SMEM)
    words = experts * (capacity + PAD)
    return pl.pallas_call(
        functools.partial(route_kernel, n_pairs, top_k, experts, capacity),
        in_specs=[smem, smem],
        out_specs=[smem, smem],
        out_shape=[jax.ShapeDtypeStruct((words,), jnp.int32), jax.ShapeDtypeStruct((words,), jnp.float32)],
        scratch_shapes=[pltpu.SMEM((experts,), jnp.int32)],
        name="route",
        interpret=INTERPRET,
    )(ids_flat, gates_flat)


def gather_kernel(n_src, with_dy, region, exp_local, capacity, chunk, nt_ref, tok_ref, gate_ref, *refs):
    stride = capacity + PAD
    token_refs = refs[:n_src]
    refs = list(refs[n_src if with_dy else n_src + 1:])
    xg_hbm = refs.pop(0)
    dy_hbm = refs.pop(0) if with_dy else None
    rows_v, buf_x, buf_g, xg_v, dy_v, xg_sem, dy_sem, tok_sem = refs
    src = pl.program_id(0)
    for k in range(n_src):
        @pl.when(src == k)
        def _(k=k):
            copy = pltpu.make_async_copy(token_refs[k], rows_v, tok_sem)
            copy.start()
            copy.wait()

    def copies(e, j, slot):
        at = pl.ds(src * chunk, chunk)
        out = [pltpu.make_async_copy(xg_v.at[slot], xg_hbm.at[e, region, j, at], xg_sem.at[slot])]
        if with_dy:
            out.append(pltpu.make_async_copy(dy_v.at[slot], dy_hbm.at[e, j, at], dy_sem.at[slot]))
        return out

    is_x = lax.broadcasted_iota(jnp.int32, (SUB, LANES), 0) < SUB // 2
    from_g = buf_g if with_dy else buf_x

    def one_expert(e, done):
        def one_chunk(j, done):
            slot = lax.rem(done, 2)

            @pl.when(done >= 2)
            def _():
                for copy in copies(e, j, slot):
                    copy.wait()

            def rows(r8, carry):
                at0 = e * stride + j * chunk + r8 * 8
                toks = [tok_ref[0, 0, at0 + u] for u in range(8)]
                gates = [gate_ref[0, 0, at0 + u] for u in range(8)]
                loaded = [rows_v[t].astype(jnp.float32) for t in toks]
                for u in range(8):
                    at = pl.ds(pl.multiple_of((r8 * 8 + u) * SUB, SUB), SUB)
                    if with_dy:
                        buf_x[at, :] = loaded[u]
                        buf_g[at, :] = loaded[u] * gates[u]
                    else:
                        buf_x[at, :] = loaded[u] * jnp.where(is_x, 1.0, gates[u])
                return carry

            lax.fori_loop(0, chunk // 8, rows, 0)
            half = SUB // 2
            for c in range(half):
                lanes = slice(c * LANES, (c + 1) * LANES)
                g_lanes = slice((half + c) * LANES, (half + c + 1) * LANES)
                xg_v[slot, :, lanes] = buf_x[pl.ds(c, chunk, stride=SUB), :].astype(jnp.bfloat16)
                xg_v[slot, :, g_lanes] = from_g[pl.ds(half + c, chunk, stride=SUB), :].astype(jnp.bfloat16)
                if with_dy:
                    dy_v[slot, :, lanes] = buf_x[pl.ds(half + c, chunk, stride=SUB), :].astype(jnp.bfloat16)
            for copy in copies(e, j, slot):
                copy.start()
            return done + 1

        return lax.fori_loop(0, nt_ref[e * 2 + region], one_chunk, done)

    lax.fori_loop(0, exp_local, one_expert, 0)
    for slot in range(2):
        for copy in copies(0, 0, slot):
            copy.wait()


def gather_rows(tokens, slot_tok, slot_gate, nt, region, capacity, carried=()):
    with_dy = region == 0
    n_src = len(tokens)
    exp_local = nt.shape[0]
    chunk = capacity // CHUNKS
    tok_dev = tokens[0].shape[0]
    width = SUB * LANES
    tile_rows = n_src * chunk
    hbm = pl.BlockSpec(memory_space=pl.ANY)
    per_src = pl.BlockSpec((1, 1, slot_tok.shape[2]), lambda s, *_: (s, 0, 0), memory_space=pltpu.SMEM)
    out_shape = [jax.ShapeDtypeStruct((exp_local, 2, CHUNKS, tile_rows, width), jnp.bfloat16)]
    if with_dy:
        out_shape.append(jax.ShapeDtypeStruct((exp_local, CHUNKS, tile_rows, width // 2), jnp.bfloat16))
    return pl.pallas_call(
        functools.partial(gather_kernel, n_src, with_dy, region, exp_local, capacity, chunk),
        grid_spec=pltpu.PrefetchScalarGridSpec(
            num_scalar_prefetch=1,
            grid=(n_src,),
            in_specs=[per_src, per_src] + [hbm] * (n_src + len(carried)),
            out_specs=[hbm] * len(out_shape),
            scratch_shapes=[
                pltpu.VMEM((tok_dev, SUB, LANES), jnp.bfloat16),
                pltpu.VMEM((chunk * SUB, LANES), jnp.float32),
                pltpu.VMEM((chunk * SUB, LANES), jnp.float32),
                pltpu.VMEM((2, chunk, width), jnp.bfloat16),
                pltpu.VMEM((2, chunk, width // 2), jnp.bfloat16),
                pltpu.SemaphoreType.DMA((2,)),
                pltpu.SemaphoreType.DMA((2,)),
                pltpu.SemaphoreType.DMA,
            ]),
        out_shape=out_shape,
        input_output_aliases={3 + n_src + k: k for k in range(len(carried))},
        compiler_params=pltpu.CompilerParams(dimension_semantics=("arbitrary",), vmem_limit_bytes=VMEM_BYTES),
        interpret=INTERPRET,
    )(nt.reshape(-1), slot_tok, slot_gate, *tokens, *carried)


def dot(a, b, dims):
    return lax.dot_general(a, b, (dims, ((), ())), preferred_element_type=jnp.float32)


NN, NT, TN = ((1,), (0,)), ((1,), (1,)), ((0,), (0,))


def expert_kernel(step_rows, nt_ref, steps_ref, meta_ref, xg_ref, dy_ref, w1o, w1p, w3o, w3p, w2o, w2p, *refs):
    *dx_refs, dr_ref = refs[len(refs) - 10 - 1 - N_OWN:-10]
    dw1_ref, dw3_ref, dw2_ref, h1, h3, da, hid, dh1, dh3, dw2t = refs[-10:]
    step = pl.program_id(0)
    code = steps_ref[meta_ref[1] + step]
    e, j = meta_ref[3 + code // CHUNKS], code % CHUNKS
    half = w1o.shape[1]
    d_model = 2 * half
    mine = pl.multiple_of(meta_ref[0] * half, half)
    other = pl.multiple_of(half - meta_ref[0] * half, half)

    @pl.when((step < meta_ref[2]) & (j == 0))
    def _():
        dw1_ref[...] = jnp.zeros_like(dw1_ref)
        dw3_ref[...] = jnp.zeros_like(dw3_ref)
        dw2t[...] = jnp.zeros_like(dw2t)

    def tile(region):
        xo = xg_ref[0, region, 0, :, pl.ds(mine, half)]
        xp = xg_ref[0, region, 0, :, pl.ds(other, half)]
        go = xg_ref[0, region, 0, :, pl.ds(d_model + mine, half)]
        gp = xg_ref[0, region, 0, :, pl.ds(d_model + other, half)]
        h1[...] = dot(xo, w1o[0], NN) + dot(xp, w1p[0], NN)
        h3[...] = dot(xo, w3o[0], NN) + dot(xp, w3p[0], NN)
        da[...] = dot(go, w2o[0], NT) + dot(gp, w2p[0], NT)

        def rows(k, carry):
            at = pl.ds(pl.multiple_of(k * step_rows, step_rows), step_rows)
            p1, p3, d = h1[at, :], h3[at, :], da[at, :]
            s = jax.nn.sigmoid(p1)
            hid[at, :] = (p1 * s * p3).astype(jnp.bfloat16)
            dh1[at, :] = (d * p3 * s * (1.0 + p1 * (1.0 - s))).astype(jnp.bfloat16)
            dh3[at, :] = (d * p1 * s).astype(jnp.bfloat16)
            return carry

        lax.fori_loop(0, h1.shape[0] // step_rows, rows, 0)
        dw1_ref[0] += dot(xo, dh1[...], TN)
        dw3_ref[0] += dot(xo, dh3[...], TN)
        dw2t[...] += dot(go, hid[...], TN)

        @pl.when(region == 0)
        def _():
            dyo = dy_ref[0, 0, :, pl.ds(mine, half)].astype(jnp.float32)
            dyp = dy_ref[0, 0, :, pl.ds(other, half)].astype(jnp.float32)
            prod = dyo * dot(hid[...], w2o[0], NN) + dyp * dot(hid[...], w2p[0], NN)
            dr = jnp.sum(prod, axis=1, keepdims=True)
            dr_ref[0, 0] = jnp.broadcast_to(dr, (dr.shape[0], LANES)).T[:1]
            dxo = (dot(dh1[...], w1o[0], NT) + dot(dh3[...], w3o[0], NT)).astype(jnp.bfloat16)
            dxp = (dot(dh1[...], w1p[0], NT) + dot(dh3[...], w3p[0], NT)).astype(jnp.bfloat16)
            chunk = dx_refs[0].shape[2]
            for k, dx_ref in enumerate(dx_refs):
                dx_ref[0, 0, :, pl.ds(mine, half)] = dxo[k * chunk:(k + 1) * chunk]
                dx_ref[0, 0, :, pl.ds(other, half)] = dxp[k * chunk:(k + 1) * chunk]

    def one_region(region, carry):
        @pl.when((step < meta_ref[2]) & (j < nt_ref[e * 2 + region]))
        def _():
            tile(region)

        return carry

    lax.fori_loop(0, 2, one_region, 0)

    @pl.when((step < meta_ref[2]) & (j == jnp.maximum(nt_ref[e * 2], nt_ref[e * 2 + 1]) - 1))
    def _():
        dw2_ref[0] = dw2t[...].T


def expert_group(e0, count, xg, dy, nt, steps, meta, own, peer, carried):
    exp_local, _, _, tile_rows, width = xg.shape
    half, d_ff = own[0].shape[1:]
    step_rows = 16
    chunk = tile_rows // N_OWN

    def place(s, steps_ref, meta_ref):
        code = steps_ref[meta_ref[1] + jnp.minimum(s, meta_ref[2] - 1)]
        return code // CHUNKS, meta_ref[3 + code // CHUNKS], code % CHUNKS

    def dy_tile(s, nt_ref, steps_ref, meta_ref):
        _, e, j = place(s, steps_ref, meta_ref)
        return (e, jnp.minimum(j, nt_ref[e * 2] - 1), 0, 0)

    def dr_tile(s, nt_ref, steps_ref, meta_ref):
        k, e, j = place(s, steps_ref, meta_ref)
        return (k, jnp.minimum(j, nt_ref[e * 2] - 1), 0, 0)

    def dx_tile(s, nt_ref, steps_ref, meta_ref):
        k, e, j = place(s, steps_ref, meta_ref)
        return (k - e0, jnp.minimum(j, nt_ref[e * 2] - 1), 0, 0)

    def xg_tile(s, nt_ref, steps_ref, meta_ref):
        _, e, j = place(s, steps_ref, meta_ref)
        return (e, 0, j, 0, 0)

    def at_own(s, nt_ref, steps_ref, meta_ref):
        return (place(s, steps_ref, meta_ref)[1], 0, 0)

    def at_peer(s, nt_ref, steps_ref, meta_ref):
        return (place(s, steps_ref, meta_ref)[0] - e0, 0, 0)

    up = lambda at: pl.BlockSpec((1, half, d_ff), at)
    down = lambda at: pl.BlockSpec((1, d_ff, half), at)
    out_shape = [
        *[jax.ShapeDtypeStruct((count, CHUNKS, chunk, width // 2), jnp.bfloat16)] * N_OWN,
        jax.ShapeDtypeStruct((exp_local, CHUNKS, 1, tile_rows), jnp.float32),
        jax.ShapeDtypeStruct((exp_local, half, d_ff), jnp.float32),
        jax.ShapeDtypeStruct((exp_local, half, d_ff), jnp.float32),
        jax.ShapeDtypeStruct((exp_local, d_ff, half), jnp.float32),
    ]
    n_in = 3 + 8
    carried = list(carried)
    return pl.pallas_call(
        functools.partial(expert_kernel, step_rows),
        grid_spec=pltpu.PrefetchScalarGridSpec(
            num_scalar_prefetch=3,
            grid=(count * CHUNKS,),
            in_specs=[
                pl.BlockSpec((1, 2, 1, tile_rows, width), xg_tile),
                pl.BlockSpec((1, 1, tile_rows, width // 2), dy_tile),
                up(at_own), up(at_peer), up(at_own), up(at_peer), down(at_own), down(at_peer),
            ] + [pl.BlockSpec(memory_space=pl.ANY)] * len(carried),
            out_specs=[
                *[pl.BlockSpec((1, 1, chunk, width // 2), dx_tile)] * N_OWN,
                pl.BlockSpec((1, 1, 1, tile_rows), dr_tile),
                up(at_own), up(at_own), down(at_own),
            ],
            scratch_shapes=[
                pltpu.VMEM((tile_rows, d_ff), jnp.float32),
                pltpu.VMEM((tile_rows, d_ff), jnp.float32),
                pltpu.VMEM((tile_rows, d_ff), jnp.float32),
                pltpu.VMEM((tile_rows, d_ff), jnp.bfloat16),
                pltpu.VMEM((tile_rows, d_ff), jnp.bfloat16),
                pltpu.VMEM((tile_rows, d_ff), jnp.bfloat16),
                pltpu.VMEM((half, d_ff), jnp.float32),
            ]),
        out_shape=out_shape,
        input_output_aliases={n_in + k: N_OWN + k for k in range(len(carried))},
        compiler_params=pltpu.CompilerParams(
            dimension_semantics=("arbitrary",), vmem_limit_bytes=VMEM_BYTES),
        interpret=INTERPRET,
    )(nt.reshape(-1), steps, meta, xg, dy, own[0], peer[0], own[1], peer[1], own[2], peer[2], *carried)


def combine_kernel(stage, counts, e0, exp_local, capacity, chunk, order_ref, tok_ref, dr_ref, *refs):
    stride = capacity + PAD
    n_exp = sum(counts)
    rows_hbm = refs[:N_OWN * len(counts)]
    refs = refs[N_OWN * len(counts):]
    first, last = stage == 0, stage == len(STAGES) - 1
    if not first:
        acc_in, refs = refs[0], refs[1:]
    if last:
        place_ref, gx_out, rg_out, acc, tmp, rows_v, sem, acc_sem = refs
    else:
        acc_out, acc, tmp, rows_v, sem, acc_sem = refs
    src = pl.program_id(0)
    tok_dev = acc.shape[0] // SUB - 1

    def expert(k, e):
        return order_ref[k * exp_local + e0 + e]

    def count_of(k, e):
        return tok_ref[(k * exp_local + expert(k, e)) * stride + capacity + 1]

    def tiles(n):
        return (n + chunk - 1) // chunk

    def start(k):
        base = 0
        for g, count in enumerate(counts):
            ref = rows_hbm[g * N_OWN + k]

            def per_expert(e, carry, ref=ref, base=base):
                def one(j, c):
                    at = (base + e) * CHUNKS + j
                    pltpu.make_async_copy(ref.at[e, j], rows_v.at[k % 2, at], sem.at[k % 2, at]).start()
                    return c

                return lax.fori_loop(0, tiles(count_of(k, base + e)), one, carry)

            lax.fori_loop(0, count, per_expert, 0)
            base += count

    @pl.when(src == 0)
    def _():
        if not first:
            load = pltpu.make_async_copy(acc_in, acc, acc_sem)
            load.start()
        start(0)
        tmp[...] = jnp.zeros_like(tmp)
        if first:
            acc[...] = jnp.zeros_like(acc)
        else:
            load.wait()

    for k in range(1, N_OWN):
        @pl.when(src == k - 1)
        def _(k=k):
            start(k)

    buf = lax.rem(src, 2)
    sub = lax.broadcasted_iota(jnp.int32, (SUB, LANES), 0)
    lane = lax.broadcasted_iota(jnp.int32, (SUB, LANES), 1)

    def per_expert(e, carry):
        n = count_of(src, e)
        here = (sub == SUB // 2) & (lane == src * exp_local + expert(src, e))

        def one(j, c):
            at = e * CHUNKS + j
            pltpu.make_async_copy(rows_hbm[0].at[0, 0], rows_v.at[buf, at], sem.at[buf, at]).wait()
            for c4 in range(SUB // 2):
                tmp[pl.ds(c4, chunk, stride=SUB), :] = rows_v[
                    buf, at, :, c4 * LANES:(c4 + 1) * LANES].astype(jnp.float32)
            slots = (src * exp_local + expert(src, e)) * stride + j * chunk
            drs = (src * n_exp + e) * capacity + j * chunk

            def rows(r8, c):
                r0 = r8 * 8
                toks = [tok_ref[slots + r0 + u] for u in range(8)]
                ats = [pl.ds(pl.multiple_of(t * SUB, SUB), SUB) for t in toks]
                sums = [acc[ats[u], :] + jnp.where(
                    here, dr_ref[drs + r0 + u], tmp[pl.ds(pl.multiple_of((r0 + u) * SUB, SUB), SUB), :])
                    for u in range(8)]
                for u in range(8):
                    acc[ats[u], :] = sums[u]
                return c

            lax.fori_loop(0, (jnp.minimum(n - j * chunk, chunk) + 7) // 8, rows, 0)
            return c

        return lax.fori_loop(0, tiles(n), one, carry)

    lax.fori_loop(0, n_exp, per_expert, 0)

    @pl.when(src == N_OWN - 1)
    def _():
        if last:
            for c in range(SUB // 2):
                gx_out[:, c * LANES:(c + 1) * LANES] = acc[pl.ds(c, tok_dev, stride=SUB), :].astype(jnp.bfloat16)
            by_expert = acc[pl.ds(SUB // 2, tok_dev, stride=SUB), :].T[:N_OWN * exp_local]
            lane_of = lax.broadcasted_iota(jnp.int32, by_expert.shape, 0)
            for k in range(place_ref.shape[0]):
                mine = jnp.where(lane_of == place_ref[k:k + 1, :], by_expert, 0.0)
                rg_out[k:k + 1, :] = jnp.sum(mine, axis=0, keepdims=True)
        else:
            store = pltpu.make_async_copy(acc, acc_out, acc_sem)
            store.start()
            store.wait()


def combine(stage, order, slot_home, dr, rows, carried, place, exp_local, capacity, tok_dev):
    counts = [GROUPS[g] for g in STAGES[stage]]
    e0 = sum(GROUPS[:STAGES[stage][0]])
    n_exp = sum(counts)
    chunk, d_model = rows[0].shape[2:]
    smem = pl.BlockSpec(memory_space=pltpu.SMEM)
    hbm = pl.BlockSpec(memory_space=pl.ANY)
    acc_shape = ((tok_dev + 1) * SUB, LANES)
    if stage == len(STAGES) - 1:
        out_specs = [pl.BlockSpec((tok_dev, d_model), lambda s: (0, 0)), pl.BlockSpec(place.shape, lambda s: (0, 0))]
        out_shape = [jax.ShapeDtypeStruct((tok_dev, d_model), jnp.bfloat16),
                     jax.ShapeDtypeStruct(place.shape, jnp.float32)]
        extra, extra_specs = [place], [pl.BlockSpec(place.shape, lambda s: (0, 0))]
    else:
        extra, extra_specs = [], []
        out_specs = [hbm]
        out_shape = [jax.ShapeDtypeStruct(acc_shape, jnp.float32)]
    return pl.pallas_call(
        functools.partial(combine_kernel, stage, counts, e0, exp_local, capacity, chunk),
        grid=(N_OWN,),
        in_specs=[smem, smem, smem] + [hbm] * (len(rows) + len(carried)) + extra_specs,
        out_specs=out_specs,
        out_shape=out_shape,
        scratch_shapes=[
            pltpu.VMEM(acc_shape, jnp.float32),
            pltpu.VMEM((chunk * SUB, LANES), jnp.float32),
            pltpu.VMEM((2, n_exp * CHUNKS, chunk, d_model), jnp.bfloat16),
            pltpu.SemaphoreType.DMA((2, n_exp * CHUNKS)),
            pltpu.SemaphoreType.DMA,
        ],
        compiler_params=pltpu.CompilerParams(
            dimension_semantics=("arbitrary",), vmem_limit_bytes=VMEM_BYTES),
        interpret=INTERPRET,
    )(order, slot_home, dr, *rows, *carried, *extra)


def solution(mesh):
    n_ep = mesh.shape["ep"]
    n_fsdp = mesh.shape["fsdp"]
    tok_spec = P(("fsdp", "ep"), None)
    spec_in = P("ep", "fsdp", None)
    spec_out = P("ep", None, "fsdp")

    def swap(value, axis, mask):
        size = n_fsdp if axis == "fsdp" else n_ep
        return lax.ppermute(value, axis, [(k, k ^ mask) for k in range(size)])

    def per_device(x_tok, dy_tok, expert_ids, route_w, w_gate, w_up, w_down):
        tok_dev, top_k = expert_ids.shape
        exp_local = w_gate.shape[0]
        experts = exp_local * n_ep
        capacity = capacity_of(tok_dev, top_k, experts)
        chunk = capacity // CHUNKS
        my_fsdp = lax.axis_index("fsdp")
        my_ep = lax.axis_index("ep")

        tokens = jnp.concatenate([x_tok, dy_tok], axis=1).reshape(tok_dev, SUB, LANES)
        tok_y = swap(tokens, "fsdp", 1)
        tok_x = swap(tokens, "ep", 2)
        tok_c = swap(tokens, "ep", 1)
        tok_yx = swap(tok_y, "ep", 2)
        tok_cx = swap(tok_x, "ep", 1)
        tok_cy = swap(tok_y, "ep", 1)
        tok_cyx = swap(tok_yx, "ep", 1)
        all_tokens = (tokens, tok_c, tok_x, tok_cx, tok_y, tok_cy, tok_yx, tok_cyx)

        slot_tok, slot_gate = route_slots(
            expert_ids.reshape(-1), route_w.reshape(-1), top_k, experts, capacity)
        slot_home = slot_tok.reshape(n_ep, -1)
        slot_home = jnp.stack(
            [lax.dynamic_index_in_dim(slot_home, my_ep ^ b, axis=0, keepdims=False) for b in range(n_ep)]).reshape(-1)
        slot_tok = lax.all_gather(slot_tok, ("fsdp", "ep"), axis=0, tiled=False)
        slot_gate = lax.all_gather(slot_gate, ("fsdp", "ep"), axis=0, tiled=False)

        def for_me(v):
            v = v.reshape(n_fsdp * n_ep, n_ep, -1)
            v = lax.dynamic_index_in_dim(v, my_ep, axis=1, keepdims=False)
            order = [(my_fsdp ^ a) * n_ep + (my_ep ^ b) for a in range(n_fsdp) for b in range(n_ep)]
            return jnp.stack([lax.dynamic_index_in_dim(v, k, axis=0, keepdims=True) for k in order])

        stride = capacity + PAD
        totals = jnp.sum(slot_tok.reshape(-1, n_ep, exp_local, stride)[..., capacity + 1], axis=0)
        totals = jnp.repeat(jnp.sum(totals.reshape(n_ep, -1, 2), axis=2), 2, axis=1)
        index = jnp.arange(exp_local, dtype=jnp.int32)
        key = jnp.where(index < GROUPS[0], 2 * n_fsdp * n_ep * capacity + 1, totals)
        ahead = (key[:, None, :] > key[:, :, None]) | (
            (key[:, None, :] == key[:, :, None]) & (index[None, None, :] < index[None, :, None]))
        rank = jnp.sum(ahead.astype(jnp.int32), axis=2)
        orders = jnp.sum(jnp.where(rank[:, None, :] == index[None, :, None], index[None, None, :], 0), axis=2)
        order_home = jnp.stack(
            [lax.dynamic_index_in_dim(orders, my_ep ^ b, axis=0, keepdims=False) for b in range(n_ep)])
        order = order_home[0]
        order_home = order_home.reshape(-1)
        word = jnp.arange(stride, dtype=jnp.int32)

        def filled(tok, empty):
            tok = tok.reshape(-1, exp_local, stride)
            held = word < tok[..., capacity + 1:capacity + 2]
            return jnp.where(held | (word == capacity + 1), tok, empty), held

        slot_tok, held = filled(for_me(slot_tok), 0)
        slot_gate = jnp.where(held, for_me(slot_gate).reshape(held.shape), 0.0)
        slot_home = filled(slot_home, tok_dev)[0].reshape(-1)
        cnt = slot_tok[..., capacity + 1].reshape(n_fsdp, n_ep, exp_local)
        slot_tok = slot_tok.reshape(n_fsdp * n_ep, 1, -1)
        slot_gate = slot_gate.reshape(n_fsdp * n_ep, 1, -1)
        most = jnp.max(cnt, axis=1)
        nt = jnp.maximum((most + chunk - 1) // chunk, 1).T
        per_expert = jnp.max(nt, axis=1)
        per_expert = jnp.sum(jnp.where(order[:, None] == index[None, :], per_expert[None, :], 0), axis=1)
        active = (jnp.arange(CHUNKS, dtype=jnp.int32) < per_expert[:, None]).reshape(-1)
        code = jnp.arange(active.shape[0], dtype=jnp.int32)
        before = jnp.sum(jnp.where((code[None, :] < code[:, None]) & active[None, :], 1, 0), axis=1)
        steps = jnp.sum(jnp.where((before[None, :] == code[:, None]) & active[None, :], code[None, :], 0), axis=1)
        first = [sum(GROUPS[:g]) for g in range(len(GROUPS))]
        n_steps = [jnp.sum(per_expert[first[g]:first[g] + GROUPS[g]]) for g in range(len(GROUPS))]
        starts = [jnp.sum(per_expert[:first[g]]) for g in range(len(GROUPS))]

        xg, dy = gather_rows(all_tokens[:n_ep], slot_tok[:n_ep], slot_gate[:n_ep], nt, 0, capacity)
        xg, = gather_rows(all_tokens[n_ep:], slot_tok[n_ep:], slot_gate[n_ep:], nt, 1, capacity, (xg,))

        own = (w_gate, w_up, w_down)
        mine = my_fsdp.astype(jnp.int32)
        place = (((expert_ids // exp_local) ^ my_ep) * exp_local + expert_ids % exp_local).T
        carried, sums = (), ()
        e0 = 0
        rows = []
        for g, count in enumerate(GROUPS):
            part = [w[:count] if g == 0 else lax.dynamic_slice_in_dim(w, order[e0], count, axis=0) for w in own]
            peer = [swap(w, "fsdp", 1) for w in part]
            meta = jnp.concatenate([jnp.stack([mine, starts[g], n_steps[g]]), order])
            out = expert_group(e0, count, xg, dy, nt, steps, meta, own, peer, carried)
            dx_g, carried = out[:n_ep], out[n_ep:]
            rows += [dx_g[0]] + [swap(dx_g[b], "ep", b) for b in range(1, n_ep)]
            e0 += count
            for stage, groups in enumerate(STAGES):
                if g == groups[-1]:
                    dr = carried[0][e0 - sum(GROUPS[k] for k in groups):e0].reshape(-1, CHUNKS, n_ep, chunk)
                    dr = dr.transpose(2, 0, 1, 3).reshape(n_ep, -1)
                    dr = jnp.concatenate(
                        [dr[0]] + [swap(dr[b], "ep", b) for b in range(1, n_ep)])
                    sums = combine(stage, order_home, slot_home, dr, rows, sums, place, exp_local, capacity, tok_dev)
                    rows = []
        _, grad_w_gate, grad_w_up, grad_w_down = carried
        grad_x, route_grad = sums[0], sums[1].T
        return grad_x, route_grad, grad_w_gate, grad_w_up, grad_w_down

    return jax.shard_map(
        per_device, mesh=mesh,
        in_specs=(tok_spec, tok_spec, tok_spec, tok_spec, spec_in, spec_in, spec_out),
        out_specs=(tok_spec, tok_spec, spec_in, spec_in, spec_out),
        check_vma=False)
```

```python
import functools

import jax
import jax.numpy as jnp
from jax import lax
from jax.experimental import pallas as pl
from jax.experimental.pallas import tpu as pltpu
from jax.sharding import PartitionSpec as P


CAP_FACTOR = 3
CHUNKS = 4
GROUPS = (4, 2, 2, 2, 2, 2, 1, 1)
STAGES = ((0, 1, 2, 3), (4, 5, 6, 7))
PAD = 8
LANES = 128
N_OWN = 4
SUB = 8
INTERPRET = False
VMEM_BYTES = 67_043_328


def capacity_of(tok_dev, top_k, experts):
    return max(8, ((CAP_FACTOR * tok_dev * top_k // experts + 7) // 8) * 8)


def route_kernel(n_pairs, top_k, experts, capacity, ids_ref, gate_ref, tok_ref, slot_gate_ref, cnt_ref):
    stride = capacity + PAD
    for e in range(experts):
        cnt_ref[e] = 0

    def step(t, carry):
        ids = [ids_ref[t * top_k + j] for j in range(top_k)]
        gates = [gate_ref[t * top_k + j] for j in range(top_k)]
        counts = [cnt_ref[e] for e in ids]
        for j in range(top_k):
            slot = ids[j] * stride + jnp.minimum(counts[j], capacity)
            tok_ref[slot] = t
            slot_gate_ref[slot] = gates[j]
            cnt_ref[ids[j]] = counts[j] + 1
        return carry

    lax.fori_loop(0, n_pairs // top_k, step, 0, unroll=2)
    for e in range(experts):
        tok_ref[e * stride + capacity + 1] = jnp.minimum(cnt_ref[e], capacity)


def route_slots(ids_flat, gates_flat, top_k, experts, capacity):
    n_pairs = ids_flat.shape[0]
    smem = pl.BlockSpec(memory_space=pltpu.SMEM)
    words = experts * (capacity + PAD)
    return pl.pallas_call(
        functools.partial(route_kernel, n_pairs, top_k, experts, capacity),
        in_specs=[smem, smem],
        out_specs=[smem, smem],
        out_shape=[jax.ShapeDtypeStruct((words,), jnp.int32), jax.ShapeDtypeStruct((words,), jnp.float32)],
        scratch_shapes=[pltpu.SMEM((experts,), jnp.int32)],
        name="route",
        interpret=INTERPRET,
    )(ids_flat, gates_flat)


def gather_kernel(n_src, with_dy, region, exp_local, capacity, chunk, nt_ref, tok_ref, gate_ref, *refs):
    stride = capacity + PAD
    token_refs = refs[:n_src]
    refs = list(refs[n_src if with_dy else n_src + 1:])
    xg_hbm = refs.pop(0)
    dy_hbm = refs.pop(0) if with_dy else None
    rows_v, buf_x, buf_g, xg_v, dy_v, xg_sem, dy_sem, tok_sem = refs
    src = pl.program_id(0)
    for k in range(n_src):
        @pl.when(src == k)
        def _(k=k):
            copy = pltpu.make_async_copy(token_refs[k], rows_v, tok_sem)
            copy.start()
            copy.wait()

    def copies(e, j, slot):
        at = pl.ds(src * chunk, chunk)
        out = [pltpu.make_async_copy(xg_v.at[slot], xg_hbm.at[e, region, j, at], xg_sem.at[slot])]
        if with_dy:
            out.append(pltpu.make_async_copy(dy_v.at[slot], dy_hbm.at[e, j, at], dy_sem.at[slot]))
        return out

    is_x = lax.broadcasted_iota(jnp.int32, (SUB, LANES), 0) < SUB // 2
    from_g = buf_g if with_dy else buf_x

    def one_expert(e, done):
        def one_chunk(j, done):
            slot = lax.rem(done, 2)

            @pl.when(done >= 2)
            def _():
                for copy in copies(e, j, slot):
                    copy.wait()

            def rows(r8, carry):
                at0 = e * stride + j * chunk + r8 * 8
                toks = [tok_ref[0, 0, at0 + u] for u in range(8)]
                gates = [gate_ref[0, 0, at0 + u] for u in range(8)]
                loaded = [rows_v[t].astype(jnp.float32) for t in toks]
                for u in range(8):
                    at = pl.ds(pl.multiple_of((r8 * 8 + u) * SUB, SUB), SUB)
                    if with_dy:
                        buf_x[at, :] = loaded[u]
                        buf_g[at, :] = loaded[u] * gates[u]
                    else:
                        buf_x[at, :] = loaded[u] * jnp.where(is_x, 1.0, gates[u])
                return carry

            lax.fori_loop(0, chunk // 8, rows, 0)
            half = SUB // 2
            for c in range(half):
                lanes = slice(c * LANES, (c + 1) * LANES)
                g_lanes = slice((half + c) * LANES, (half + c + 1) * LANES)
                xg_v[slot, :, lanes] = buf_x[pl.ds(c, chunk, stride=SUB), :].astype(jnp.bfloat16)
                xg_v[slot, :, g_lanes] = from_g[pl.ds(half + c, chunk, stride=SUB), :].astype(jnp.bfloat16)
                if with_dy:
                    dy_v[slot, :, lanes] = buf_x[pl.ds(half + c, chunk, stride=SUB), :].astype(jnp.bfloat16)
            for copy in copies(e, j, slot):
                copy.start()
            return done + 1

        return lax.fori_loop(0, nt_ref[e * 2 + region], one_chunk, done)

    lax.fori_loop(0, exp_local, one_expert, 0)
    for slot in range(2):
        for copy in copies(0, 0, slot):
            copy.wait()


def gather_rows(tokens, slot_tok, slot_gate, nt, region, capacity, carried=()):
    with_dy = region == 0
    n_src = len(tokens)
    exp_local = nt.shape[0]
    chunk = capacity // CHUNKS
    tok_dev = tokens[0].shape[0]
    width = SUB * LANES
    tile_rows = n_src * chunk
    hbm = pl.BlockSpec(memory_space=pl.ANY)
    per_src = pl.BlockSpec((1, 1, slot_tok.shape[2]), lambda s, *_: (s, 0, 0), memory_space=pltpu.SMEM)
    out_shape = [jax.ShapeDtypeStruct((exp_local, 2, CHUNKS, tile_rows, width), jnp.bfloat16)]
    if with_dy:
        out_shape.append(jax.ShapeDtypeStruct((exp_local, CHUNKS, tile_rows, width // 2), jnp.bfloat16))
    return pl.pallas_call(
        functools.partial(gather_kernel, n_src, with_dy, region, exp_local, capacity, chunk),
        grid_spec=pltpu.PrefetchScalarGridSpec(
            num_scalar_prefetch=1,
            grid=(n_src,),
            in_specs=[per_src, per_src] + [hbm] * (n_src + len(carried)),
            out_specs=[hbm] * len(out_shape),
            scratch_shapes=[
                pltpu.VMEM((tok_dev, SUB, LANES), jnp.bfloat16),
                pltpu.VMEM((chunk * SUB, LANES), jnp.float32),
                pltpu.VMEM((chunk * SUB, LANES), jnp.float32),
                pltpu.VMEM((2, chunk, width), jnp.bfloat16),
                pltpu.VMEM((2, chunk, width // 2), jnp.bfloat16),
                pltpu.SemaphoreType.DMA((2,)),
                pltpu.SemaphoreType.DMA((2,)),
                pltpu.SemaphoreType.DMA,
            ]),
        out_shape=out_shape,
        input_output_aliases={3 + n_src + k: k for k in range(len(carried))},
        compiler_params=pltpu.CompilerParams(dimension_semantics=("arbitrary",), vmem_limit_bytes=VMEM_BYTES),
        interpret=INTERPRET,
    )(nt.reshape(-1), slot_tok, slot_gate, *tokens, *carried)


def dot(a, b, dims):
    return lax.dot_general(a, b, (dims, ((), ())), preferred_element_type=jnp.float32)


NN, NT, TN = ((1,), (0,)), ((1,), (1,)), ((0,), (0,))


def expert_kernel(g, step_rows, nt_ref, steps_ref, meta_ref, xg_ref, dy_ref, w1o, w1p, w3o, w3p, w2o, w2p, *refs):
    *dx_refs, dr_ref = refs[len(refs) - 10 - 1 - N_OWN:-10]
    dw1_ref, dw3_ref, dw2_ref, h1, h3, da, hid, dh1, dh3, dw2t = refs[-10:]
    step = pl.program_id(0)
    n_groups = len(GROUPS)
    n_steps = meta_ref[1 + n_groups + g]
    code = steps_ref[meta_ref[1 + g] + step]
    e, j = meta_ref[1 + 2 * n_groups + code // CHUNKS], code % CHUNKS
    half = w1o.shape[1]
    d_model = 2 * half
    mine = pl.multiple_of(meta_ref[0] * half, half)
    other = pl.multiple_of(half - meta_ref[0] * half, half)

    @pl.when((step < n_steps) & (j == 0))
    def _():
        dw1_ref[...] = jnp.zeros_like(dw1_ref)
        dw3_ref[...] = jnp.zeros_like(dw3_ref)
        dw2t[...] = jnp.zeros_like(dw2t)

    def tile(region):
        xo = xg_ref[0, region, 0, :, pl.ds(mine, half)]
        xp = xg_ref[0, region, 0, :, pl.ds(other, half)]
        go = xg_ref[0, region, 0, :, pl.ds(d_model + mine, half)]
        gp = xg_ref[0, region, 0, :, pl.ds(d_model + other, half)]
        h1[...] = dot(xo, w1o[0], NN) + dot(xp, w1p[0], NN)
        h3[...] = dot(xo, w3o[0], NN) + dot(xp, w3p[0], NN)
        da[...] = dot(go, w2o[0], NT) + dot(gp, w2p[0], NT)

        def rows(k, carry):
            at = pl.ds(pl.multiple_of(k * step_rows, step_rows), step_rows)
            p1, p3, d = h1[at, :], h3[at, :], da[at, :]
            s = jax.nn.sigmoid(p1)
            hid[at, :] = (p1 * s * p3).astype(jnp.bfloat16)
            dh1[at, :] = (d * p3 * s * (1.0 + p1 * (1.0 - s))).astype(jnp.bfloat16)
            dh3[at, :] = (d * p1 * s).astype(jnp.bfloat16)
            return carry

        lax.fori_loop(0, h1.shape[0] // step_rows, rows, 0)
        dw1_ref[0] += dot(xo, dh1[...], TN)
        dw3_ref[0] += dot(xo, dh3[...], TN)
        dw2t[...] += dot(go, hid[...], TN)

        @pl.when(region == 0)
        def _():
            dyo = dy_ref[0, 0, :, pl.ds(mine, half)].astype(jnp.float32)
            dyp = dy_ref[0, 0, :, pl.ds(other, half)].astype(jnp.float32)
            prod = dyo * dot(hid[...], w2o[0], NN) + dyp * dot(hid[...], w2p[0], NN)
            dr = jnp.sum(prod, axis=1, keepdims=True)
            dr_ref[0, 0] = jnp.broadcast_to(dr, (dr.shape[0], LANES)).T[:1]
            dxo = (dot(dh1[...], w1o[0], NT) + dot(dh3[...], w3o[0], NT)).astype(jnp.bfloat16)
            dxp = (dot(dh1[...], w1p[0], NT) + dot(dh3[...], w3p[0], NT)).astype(jnp.bfloat16)
            chunk = dx_refs[0].shape[2]
            for k, dx_ref in enumerate(dx_refs):
                dx_ref[0, 0, :, pl.ds(mine, half)] = dxo[k * chunk:(k + 1) * chunk]
                dx_ref[0, 0, :, pl.ds(other, half)] = dxp[k * chunk:(k + 1) * chunk]

    def one_region(region, carry):
        @pl.when((step < n_steps) & (j < nt_ref[e * 2 + region]))
        def _():
            tile(region)

        return carry

    lax.fori_loop(0, 2, one_region, 0)

    @pl.when((step < n_steps) & (j == jnp.maximum(nt_ref[e * 2], nt_ref[e * 2 + 1]) - 1))
    def _():
        dw2_ref[0] = dw2t[...].T


def expert_group(g, e0, count, xg, dy, nt, steps, meta, own, peer, carried):
    exp_local, _, _, tile_rows, width = xg.shape
    half, d_ff = own[0].shape[1:]
    n_groups = len(GROUPS)
    step_rows = 16
    chunk = tile_rows // N_OWN

    def place(s, steps_ref, meta_ref):
        code = steps_ref[meta_ref[1 + g] + jnp.minimum(s, meta_ref[1 + n_groups + g] - 1)]
        return code // CHUNKS, meta_ref[1 + 2 * n_groups + code // CHUNKS], code % CHUNKS

    def dy_tile(s, nt_ref, steps_ref, meta_ref):
        _, e, j = place(s, steps_ref, meta_ref)
        return (e, jnp.minimum(j, nt_ref[e * 2] - 1), 0, 0)

    def dr_tile(s, nt_ref, steps_ref, meta_ref):
        k, e, j = place(s, steps_ref, meta_ref)
        return (k, jnp.minimum(j, nt_ref[e * 2] - 1), 0, 0)

    def dx_tile(s, nt_ref, steps_ref, meta_ref):
        k, e, j = place(s, steps_ref, meta_ref)
        return (k - e0, jnp.minimum(j, nt_ref[e * 2] - 1), 0, 0)

    def xg_tile(s, nt_ref, steps_ref, meta_ref):
        _, e, j = place(s, steps_ref, meta_ref)
        return (e, 0, j, 0, 0)

    def at_own(s, nt_ref, steps_ref, meta_ref):
        return (place(s, steps_ref, meta_ref)[1], 0, 0)

    def at_peer(s, nt_ref, steps_ref, meta_ref):
        return (place(s, steps_ref, meta_ref)[0] - e0, 0, 0)

    up = lambda at: pl.BlockSpec((1, half, d_ff), at)
    down = lambda at: pl.BlockSpec((1, d_ff, half), at)
    out_shape = [
        *[jax.ShapeDtypeStruct((count, CHUNKS, chunk, width // 2), jnp.bfloat16)] * N_OWN,
        jax.ShapeDtypeStruct((exp_local, CHUNKS, 1, tile_rows), jnp.float32),
        jax.ShapeDtypeStruct((exp_local, half, d_ff), jnp.float32),
        jax.ShapeDtypeStruct((exp_local, half, d_ff), jnp.float32),
        jax.ShapeDtypeStruct((exp_local, d_ff, half), jnp.float32),
    ]
    n_in = 3 + 8
    carried = list(carried)
    return pl.pallas_call(
        functools.partial(expert_kernel, g, step_rows),
        grid_spec=pltpu.PrefetchScalarGridSpec(
            num_scalar_prefetch=3,
            grid=(count * CHUNKS,),
            in_specs=[
                pl.BlockSpec((1, 2, 1, tile_rows, width), xg_tile),
                pl.BlockSpec((1, 1, tile_rows, width // 2), dy_tile),
                up(at_own), up(at_peer), up(at_own), up(at_peer), down(at_own), down(at_peer),
            ] + [pl.BlockSpec(memory_space=pl.ANY)] * len(carried),
            out_specs=[
                *[pl.BlockSpec((1, 1, chunk, width // 2), dx_tile)] * N_OWN,
                pl.BlockSpec((1, 1, 1, tile_rows), dr_tile),
                up(at_own), up(at_own), down(at_own),
            ],
            scratch_shapes=[
                pltpu.VMEM((tile_rows, d_ff), jnp.float32),
                pltpu.VMEM((tile_rows, d_ff), jnp.float32),
                pltpu.VMEM((tile_rows, d_ff), jnp.float32),
                pltpu.VMEM((tile_rows, d_ff), jnp.bfloat16),
                pltpu.VMEM((tile_rows, d_ff), jnp.bfloat16),
                pltpu.VMEM((tile_rows, d_ff), jnp.bfloat16),
                pltpu.VMEM((half, d_ff), jnp.float32),
            ]),
        out_shape=out_shape,
        input_output_aliases={n_in + k: N_OWN + k for k in range(len(carried))},
        compiler_params=pltpu.CompilerParams(
            dimension_semantics=("arbitrary",), vmem_limit_bytes=VMEM_BYTES),
        interpret=INTERPRET,
    )(nt.reshape(-1), steps, meta, xg, dy, own[0], peer[0], own[1], peer[1], own[2], peer[2], *carried)


def combine_kernel(stage, counts, e0, exp_local, capacity, chunk, order_ref, tok_ref, dr_ref, *refs):
    stride = capacity + PAD
    n_exp = sum(counts)
    rows_hbm = refs[:N_OWN * len(counts)]
    refs = refs[N_OWN * len(counts):]
    first, last = stage == 0, stage == len(STAGES) - 1
    if not first:
        acc_in, refs = refs[0], refs[1:]
    if last:
        place_ref, gx_out, rg_out, acc, tmp, rows_v, sem, acc_sem = refs
    else:
        acc_out, acc, tmp, rows_v, sem, acc_sem = refs
    src = pl.program_id(0)
    tok_dev = acc.shape[0] // SUB - 1

    def expert(k, e):
        return order_ref[k * exp_local + e0 + e]

    def count_of(k, e):
        return tok_ref[(k * exp_local + expert(k, e)) * stride + capacity + 1]

    def tiles(n):
        return (n + chunk - 1) // chunk

    def start(k):
        base = 0
        for g, count in enumerate(counts):
            ref = rows_hbm[g * N_OWN + k]

            def per_expert(e, carry, ref=ref, base=base):
                def one(j, c):
                    at = (base + e) * CHUNKS + j
                    pltpu.make_async_copy(ref.at[e, j], rows_v.at[k % 2, at], sem.at[k % 2, at]).start()
                    return c

                return lax.fori_loop(0, tiles(count_of(k, base + e)), one, carry)

            lax.fori_loop(0, count, per_expert, 0)
            base += count

    @pl.when(src == 0)
    def _():
        if not first:
            load = pltpu.make_async_copy(acc_in, acc, acc_sem)
            load.start()
        start(0)
        tmp[...] = jnp.zeros_like(tmp)
        if first:
            acc[...] = jnp.zeros_like(acc)
        else:
            load.wait()

    for k in range(1, N_OWN):
        @pl.when(src == k - 1)
        def _(k=k):
            start(k)

    buf = lax.rem(src, 2)
    sub = lax.broadcasted_iota(jnp.int32, (SUB, LANES), 0)
    lane = lax.broadcasted_iota(jnp.int32, (SUB, LANES), 1)

    def per_expert(e, carry):
        n = count_of(src, e)
        here = (sub == SUB // 2) & (lane == src * exp_local + expert(src, e))

        def one(j, c):
            at = e * CHUNKS + j
            pltpu.make_async_copy(rows_hbm[0].at[0, 0], rows_v.at[buf, at], sem.at[buf, at]).wait()
            for c4 in range(SUB // 2):
                tmp[pl.ds(c4, chunk, stride=SUB), :] = rows_v[
                    buf, at, :, c4 * LANES:(c4 + 1) * LANES].astype(jnp.float32)
            slots = (src * exp_local + expert(src, e)) * stride + j * chunk
            drs = (src * n_exp + e) * capacity + j * chunk

            def rows(r8, c):
                r0 = r8 * 8
                toks = [tok_ref[slots + r0 + u] for u in range(8)]
                ats = [pl.ds(pl.multiple_of(t * SUB, SUB), SUB) for t in toks]
                sums = [acc[ats[u], :] + jnp.where(
                    here, dr_ref[drs + r0 + u], tmp[pl.ds(pl.multiple_of((r0 + u) * SUB, SUB), SUB), :])
                    for u in range(8)]
                for u in range(8):
                    acc[ats[u], :] = sums[u]
                return c

            lax.fori_loop(0, (jnp.minimum(n - j * chunk, chunk) + 7) // 8, rows, 0)
            return c

        return lax.fori_loop(0, tiles(n), one, carry)

    lax.fori_loop(0, n_exp, per_expert, 0)

    @pl.when(src == N_OWN - 1)
    def _():
        if last:
            for c in range(SUB // 2):
                gx_out[:, c * LANES:(c + 1) * LANES] = acc[pl.ds(c, tok_dev, stride=SUB), :].astype(jnp.bfloat16)
            by_expert = acc[pl.ds(SUB // 2, tok_dev, stride=SUB), :].T[:N_OWN * exp_local]
            lane_of = lax.broadcasted_iota(jnp.int32, by_expert.shape, 0)
            for k in range(place_ref.shape[0]):
                mine = jnp.where(lane_of == place_ref[k:k + 1, :], by_expert, 0.0)
                rg_out[k:k + 1, :] = jnp.sum(mine, axis=0, keepdims=True)
        else:
            store = pltpu.make_async_copy(acc, acc_out, acc_sem)
            store.start()
            store.wait()


def combine(stage, order, slot_home, dr, rows, carried, place, exp_local, capacity, tok_dev):
    counts = [GROUPS[g] for g in STAGES[stage]]
    e0 = sum(GROUPS[:STAGES[stage][0]])
    n_exp = sum(counts)
    chunk, d_model = rows[0].shape[2:]
    smem = pl.BlockSpec(memory_space=pltpu.SMEM)
    hbm = pl.BlockSpec(memory_space=pl.ANY)
    acc_shape = ((tok_dev + 1) * SUB, LANES)
    if stage == len(STAGES) - 1:
        out_specs = [pl.BlockSpec((tok_dev, d_model), lambda s: (0, 0)), pl.BlockSpec(place.shape, lambda s: (0, 0))]
        out_shape = [jax.ShapeDtypeStruct((tok_dev, d_model), jnp.bfloat16),
                     jax.ShapeDtypeStruct(place.shape, jnp.float32)]
        extra, extra_specs = [place], [pl.BlockSpec(place.shape, lambda s: (0, 0))]
    else:
        extra, extra_specs = [], []
        out_specs = [hbm]
        out_shape = [jax.ShapeDtypeStruct(acc_shape, jnp.float32)]
    return pl.pallas_call(
        functools.partial(combine_kernel, stage, counts, e0, exp_local, capacity, chunk),
        grid=(N_OWN,),
        in_specs=[smem, smem, smem] + [hbm] * (len(rows) + len(carried)) + extra_specs,
        out_specs=out_specs,
        out_shape=out_shape,
        scratch_shapes=[
            pltpu.VMEM(acc_shape, jnp.float32),
            pltpu.VMEM((chunk * SUB, LANES), jnp.float32),
            pltpu.VMEM((2, n_exp * CHUNKS, chunk, d_model), jnp.bfloat16),
            pltpu.SemaphoreType.DMA((2, n_exp * CHUNKS)),
            pltpu.SemaphoreType.DMA,
        ],
        compiler_params=pltpu.CompilerParams(
            dimension_semantics=("arbitrary",), vmem_limit_bytes=VMEM_BYTES),
        interpret=INTERPRET,
    )(order, slot_home, dr, *rows, *carried, *extra)


def solution(mesh):
    n_ep = mesh.shape["ep"]
    n_fsdp = mesh.shape["fsdp"]
    tok_spec = P(("fsdp", "ep"), None)
    spec_in = P("ep", "fsdp", None)
    spec_out = P("ep", None, "fsdp")

    def swap(value, axis, mask):
        size = n_fsdp if axis == "fsdp" else n_ep
        return lax.ppermute(value, axis, [(k, k ^ mask) for k in range(size)])

    def per_device(x_tok, dy_tok, expert_ids, route_w, w_gate, w_up, w_down):
        tok_dev, top_k = expert_ids.shape
        exp_local = w_gate.shape[0]
        experts = exp_local * n_ep
        capacity = capacity_of(tok_dev, top_k, experts)
        chunk = capacity // CHUNKS
        my_fsdp = lax.axis_index("fsdp")
        my_ep = lax.axis_index("ep")

        tokens = jnp.concatenate([x_tok, dy_tok], axis=1).reshape(tok_dev, SUB, LANES)
        tok_y = swap(tokens, "fsdp", 1)
        tok_x = swap(tokens, "ep", 2)
        tok_c = swap(tokens, "ep", 1)
        tok_yx = swap(tok_y, "ep", 2)
        tok_cx = swap(tok_x, "ep", 1)
        tok_cy = swap(tok_y, "ep", 1)
        tok_cyx = swap(tok_yx, "ep", 1)
        all_tokens = (tokens, tok_c, tok_x, tok_cx, tok_y, tok_cy, tok_yx, tok_cyx)

        slot_tok, slot_gate = route_slots(
            expert_ids.reshape(-1), route_w.reshape(-1), top_k, experts, capacity)
        slot_home = slot_tok.reshape(n_ep, -1)
        slot_home = jnp.stack(
            [lax.dynamic_index_in_dim(slot_home, my_ep ^ b, axis=0, keepdims=False) for b in range(n_ep)]).reshape(-1)
        slot_tok = lax.all_gather(slot_tok, ("fsdp", "ep"), axis=0, tiled=False)
        slot_gate = lax.all_gather(slot_gate, ("fsdp", "ep"), axis=0, tiled=False)

        def for_me(v):
            v = v.reshape(n_fsdp * n_ep, n_ep, -1)
            v = lax.dynamic_index_in_dim(v, my_ep, axis=1, keepdims=False)
            order = [(my_fsdp ^ a) * n_ep + (my_ep ^ b) for a in range(n_fsdp) for b in range(n_ep)]
            return jnp.stack([lax.dynamic_index_in_dim(v, k, axis=0, keepdims=True) for k in order])

        stride = capacity + PAD
        totals = jnp.sum(slot_tok.reshape(-1, n_ep, exp_local, stride)[..., capacity + 1], axis=0)
        totals = jnp.repeat(jnp.sum(totals.reshape(n_ep, -1, 2), axis=2), 2, axis=1)
        index = jnp.arange(exp_local, dtype=jnp.int32)
        key = jnp.where(index < GROUPS[0], 2 * n_fsdp * n_ep * capacity + 1, totals)
        ahead = (key[:, None, :] > key[:, :, None]) | (
            (key[:, None, :] == key[:, :, None]) & (index[None, None, :] < index[None, :, None]))
        rank = jnp.sum(ahead.astype(jnp.int32), axis=2)
        orders = jnp.sum(jnp.where(rank[:, None, :] == index[None, :, None], index[None, None, :], 0), axis=2)
        order_home = jnp.stack(
            [lax.dynamic_index_in_dim(orders, my_ep ^ b, axis=0, keepdims=False) for b in range(n_ep)])
        order = order_home[0]
        order_home = order_home.reshape(-1)
        word = jnp.arange(stride, dtype=jnp.int32)

        def filled(tok, empty):
            tok = tok.reshape(-1, exp_local, stride)
            held = word < tok[..., capacity + 1:capacity + 2]
            return jnp.where(held | (word == capacity + 1), tok, empty), held

        slot_tok, held = filled(for_me(slot_tok), 0)
        slot_gate = jnp.where(held, for_me(slot_gate).reshape(held.shape), 0.0)
        slot_home = filled(slot_home, tok_dev)[0].reshape(-1)
        cnt = slot_tok[..., capacity + 1].reshape(n_fsdp, n_ep, exp_local)
        slot_tok = slot_tok.reshape(n_fsdp * n_ep, 1, -1)
        slot_gate = slot_gate.reshape(n_fsdp * n_ep, 1, -1)
        most = jnp.max(cnt, axis=1)
        nt = jnp.maximum((most + chunk - 1) // chunk, 1).T
        per_expert = jnp.max(nt, axis=1)
        per_expert = jnp.sum(jnp.where(order[:, None] == index[None, :], per_expert[None, :], 0), axis=1)
        active = (jnp.arange(CHUNKS, dtype=jnp.int32) < per_expert[:, None]).reshape(-1)
        code = jnp.arange(active.shape[0], dtype=jnp.int32)
        before = jnp.sum(jnp.where((code[None, :] < code[:, None]) & active[None, :], 1, 0), axis=1)
        steps = jnp.sum(jnp.where((before[None, :] == code[:, None]) & active[None, :], code[None, :], 0), axis=1)
        bounds = jnp.array([sum(GROUPS[:g]) for g in range(len(GROUPS) + 1)], jnp.int32)
        starts = jnp.sum(jnp.where(index[None, :] < bounds[:, None], per_expert[None, :], 0), axis=1)

        xg, dy = gather_rows(all_tokens[:n_ep], slot_tok[:n_ep], slot_gate[:n_ep], nt, 0, capacity)
        xg, = gather_rows(all_tokens[n_ep:], slot_tok[n_ep:], slot_gate[n_ep:], nt, 1, capacity, (xg,))

        own = (w_gate, w_up, w_down)
        meta = jnp.concatenate([my_fsdp.astype(jnp.int32)[None], starts[:-1], starts[1:] - starts[:-1], order])
        place = (((expert_ids // exp_local) ^ my_ep) * exp_local + expert_ids % exp_local).T
        carried, sums = (), ()
        e0 = 0
        rows = []
        for g, count in enumerate(GROUPS):
            part = [w[:count] if g == 0 else lax.dynamic_slice_in_dim(w, order[e0], count, axis=0) for w in own]
            peer = [swap(w, "fsdp", 1) for w in part]
            out = expert_group(g, e0, count, xg, dy, nt, steps, meta, own, peer, carried)
            dx_g, carried = out[:n_ep], out[n_ep:]
            rows += [dx_g[0]] + [swap(dx_g[b], "ep", b) for b in range(1, n_ep)]
            e0 += count
            for stage, groups in enumerate(STAGES):
                if g == groups[-1]:
                    dr = carried[0][e0 - sum(GROUPS[k] for k in groups):e0].reshape(-1, CHUNKS, n_ep, chunk)
                    dr = dr.transpose(2, 0, 1, 3).reshape(n_ep, -1)
                    dr = jnp.concatenate(
                        [dr[0]] + [swap(dr[b], "ep", b) for b in range(1, n_ep)])
                    sums = combine(stage, order_home, slot_home, dr, rows, sums, place, exp_local, capacity, tok_dev)
                    rows = []
        _, grad_w_gate, grad_w_up, grad_w_down = carried
        grad_x, route_grad = sums[0], sums[1].T
        return grad_x, route_grad, grad_w_gate, grad_w_up, grad_w_down

    return jax.shard_map(
        per_device, mesh=mesh,
        in_specs=(tok_spec, tok_spec, tok_spec, tok_spec, spec_in, spec_in, spec_out),
        out_specs=(tok_spec, tok_spec, spec_in, spec_in, spec_out),
        check_vma=False)
```
